512 devices in a mesh: rows: 128 (over z, y, core), cols: 4 (over x).
Axes of the slice: x: 4, y: 4, z: 16, core: 2. Of those that a mesh axis runs over, the one named last changes fastest.
Arguments:
- blocks: bfloat16 [512, 4, 3, 128, 128], P('rows', 'cols'), may hold values from -1.1953125 to 1.1953125
- block_cols: int32 [512, 4, 3], P('rows', 'cols'), may hold values from 0 to 511, as said below
Outputs:
- square_blocks: bfloat16 [512, 4, 36, 128, 128], P('rows', 'cols')
- square_cols: int32 [512, 4, 36], P('rows', 'cols')
- square_start: int32 [512, 4], P('rows', 'cols')
The draws below stay inside these ranges and needn't reach their ends.
Inputs may be any that keep to these rules, and one draw needn't show every extreme that they name: Block-row i lies in panel p = i // 4; every block_cols[i, g, s] is a block-column congruent to g modulo 4 among block-rows 4 * (p - 4) to 4 * (p + 4) - 1, taken modulo 512; the three entries of one group differ; the block-columns i - 1, i and i + 1 (modulo 512) are always among a row's entries.
All inputs are finite; a program needn't handle non-finite values.
Results may differ from the reference program's by a relative error of at most 0.001.
Values may be sent and summed in bfloat16 or wider, within the bound.
No kernel may reach another device: no remote copies, remote signals or barrier semaphores. Data moves between devices by JAX's collectives and lax.ppermute only.
A program may use at most 64 MiB of HBM per device.

```python
import jax
import jax.numpy as jnp
from jax import lax

BS = 128
PB = 4
KG = 3
HP = 4
GROUPS = 4
NB = 512
K = 12


def draw_block_cols(key, part):
    row_ids = jnp.arange(NB, dtype=jnp.int32)
    panel = row_ids // PB
    window_base = (panel - HP) * PB % NB
    choices_count = 2 * HP * PB // GROUPS
    group_ids = jnp.arange(GROUPS, dtype=jnp.int32)
    residue = (group_ids[None, :] - window_base[:, None]) % GROUPS
    delta = (group_ids[None, :] - row_ids[:, None] + 1) % GROUPS
    has_band = delta <= 2
    band_col = (row_ids[:, None] - 1 + delta) % NB
    band_place = (band_col - window_base[:, None]) % NB // GROUPS
    key_pick = jax.random.fold_in(key, 11)
    key_jump = jax.random.fold_in(key, 23)
    key_extra = jax.random.fold_in(key, 37)
    picked = jax.random.randint(key_pick, (NB, GROUPS), 0, choices_count, dtype=jnp.int32)
    jumped = jax.random.randint(key_jump, (NB, GROUPS), 1, choices_count, dtype=jnp.int32)
    extra = jax.random.randint(key_extra, (NB, GROUPS), 1, choices_count - 1, dtype=jnp.int32)
    other_jump = 1 + (jumped - 1 + extra) % (choices_count - 1)
    first_place = jnp.where(has_band, band_place, picked)
    second_place = (first_place + jumped) % choices_count
    third_place = (first_place + other_jump) % choices_count
    first_col = (window_base[:, None] + first_place * GROUPS + residue) % NB
    second_col = (window_base[:, None] + second_place * GROUPS + residue) % NB
    third_col = (window_base[:, None] + third_place * GROUPS + residue) % NB
    return jnp.stack([first_col, second_col, third_col], axis=-1).astype(jnp.int32)


def steps_of(stream_key, shape, shards, low, high):
    level = 1.0
    for axis_at, shards_of in shards:
        draws = jax.random.uniform(jax.random.fold_in(jax.random.fold_in(stream_key, 6), axis_at), (shards_of,), jnp.float32, low / len(shards), high / len(shards))
        level = level * jnp.repeat(jnp.exp(draws), shape[axis_at] // shards_of).reshape((-1,) + (1,) * (len(shape) - 1 - axis_at))
    return level


def centred(rng, shape, deviation, bound, shards=(), kind=jnp.bfloat16):
    result = deviation * jax.random.normal(rng, shape, jnp.float32)
    if shards:
        result = result * steps_of(rng, shape, shards, -0.22, 0.18)
    return jnp.clip(result, -bound, bound).astype(kind)


def setup_inputs(seed: int = 0) -> dict:
    key_of = jax.random.split(jax.random.key(seed), 3)
    blocks = centred(key_of[0], (NB, GROUPS, KG, BS, BS), 0.2, 1.1953125, ((0, 128), (1, 4)))
    block_cols = draw_block_cols(jax.random.fold_in(key_of[2], 71), 0)
    return dict(blocks=blocks, block_cols=block_cols)


def unique_slots(candidates):
    width = candidates.shape[-1]
    ordered = jnp.sort(candidates, axis=-1)
    firsts = jnp.concatenate([jnp.ones(ordered.shape[:-1] + (1,), dtype=bool), ordered[..., 1:] != ordered[..., :-1]], axis=-1)
    marks = firsts.astype(jnp.int32)
    totals = jnp.sum(marks, axis=-1).astype(jnp.int32)
    ranking = jnp.sum(marks[..., None, :] * (ordered[..., None, :] < candidates[..., :, None]).astype(jnp.int32), axis=-1)
    places = jnp.cumsum(marks, axis=-1) - 1
    slot_ids = jnp.arange(width, dtype=jnp.int32)
    chosen = (places[..., None, :] == slot_ids[:, None]) & firsts[..., None, :]
    columns = jnp.sum(jnp.where(chosen, ordered[..., None, :], 0), axis=-1).astype(jnp.int32)
    columns = jnp.where(slot_ids < totals[..., None], columns, -1).astype(jnp.int32)
    onehot = (ranking[..., None, :] == slot_ids[:, None]).astype(jnp.float32)
    return columns, onehot, totals


def reference(blocks, block_cols):
    def one_row(row_index):
        named = block_cols[row_index].reshape(K).astype(jnp.int32)
        left = blocks[row_index].reshape(K, BS, BS).astype(jnp.float32)
        right_vals = blocks[named].astype(jnp.float32)
        right_cols = block_cols[named]
        products = jnp.einsum("tab,tgsbc->gtsac", left, right_vals, precision=lax.Precision.HIGHEST)
        candidates = jnp.transpose(right_cols, (1, 0, 2)).reshape(GROUPS, K * KG)
        columns, onehot, totals = unique_slots(candidates)
        merged = jnp.einsum("goq,gqac->goac", onehot, products.reshape(GROUPS, K * KG, BS, BS), precision=lax.Precision.HIGHEST)
        return merged.astype(jnp.bfloat16), columns, totals

    square_blocks, square_cols, counts = lax.map(one_row, jnp.arange(NB, dtype=jnp.int32))
    square_start = (jnp.cumsum(counts, axis=0) - counts).astype(jnp.int32)
    return square_blocks, square_cols, square_start
```

```python
import jax
import jax.numpy as jnp
from jax import lax
from jax.experimental import pallas as pl
from jax.experimental.pallas import tpu as pltpu
from jax.sharding import Mesh
from jax.sharding import PartitionSpec as P

HP = 4
PB = 4
KG = 3
GROUPS = 4
BS = 128
NP = 128
WIDTH = 36
USED = 15
WIN = 2 * HP
ROWS = ("rows_0", "rows_1", "rows_2")
SLOTS = ((4, 5, 2, 3, 6, 7, 0, 1), (4, 3, 2, 1, 6, 5, 0, 7))


def place():
    return lax.axis_index(ROWS), lax.axis_index("cols")


def index_kernel(tab_ref, cols_ref, starts_ref, map_ref, pres_ref):
    p0, c = place()
    table = tab_ref[...]
    j_of = lax.broadcasted_iota(jnp.int32, (NP, BS), 1)
    panel_of = lax.broadcasted_iota(jnp.int32, (NP, BS), 0)
    one = jnp.float32(1)
    zero = jnp.float32(0)
    rights = []
    for r in range(PB):
        hit = None
        for s in range(KG):
            col = jnp.zeros((NP, 1), jnp.int32)
            for g in range(GROUPS):
                at = 12 * g + KG * r + s
                col = jnp.where(c == g, table[:, at : at + 1], col)
            same = lax.shift_right_logical(col, 2) == j_of
            hit = same if hit is None else hit | same
        rights.append(jnp.where(hit, one, zero).astype(jnp.bfloat16))
    right = jnp.concatenate(rights, axis=0)
    lane = lax.broadcasted_iota(jnp.int32, (NP, PB * NP), 1)
    row_of_lane = 4 * (lane & (NP - 1)) + lax.shift_right_logical(lane, 7)
    every = jnp.zeros((NP, BS), jnp.float32)
    for r in range(PB):
        hit = None
        for g in range(GROUPS):
            for s in range(KG):
                at = 12 * g + KG * r + s
                same = table[:, at : at + 1] == row_of_lane
                hit = same if hit is None else hit | same
        left = jnp.where(hit, one, zero).astype(jnp.bfloat16)
        paths = jnp.dot(left, right, preferred_element_type=jnp.float32)
        present = jnp.where(paths > 0.5, one, zero)
        pres_ref[r] = present
        every = every + present
    before = jnp.sum(jnp.where(panel_of < p0, every, zero)).astype(jnp.int32)
    own = [pres_ref[r, pl.ds(p0, 1), :] for r in range(PB)]
    own = jnp.concatenate(own + own, axis=0)
    upper = jnp.where(panel_of < j_of, one, zero).astype(jnp.bfloat16)
    rank = jnp.dot(own.astype(jnp.bfloat16), upper, preferred_element_type=jnp.float32)
    rank = rank.astype(jnp.int32)
    slot = lax.broadcasted_iota(jnp.int32, (40, BS), 0)
    js = lax.broadcasted_iota(jnp.int32, (8, BS), 1).astype(jnp.bfloat16)
    row = lax.broadcasted_iota(jnp.int32, (PB, 1), 0)
    starts = jnp.zeros((PB, 1), jnp.int32) + before
    for r in range(PB):
        taken = (rank[r : r + 1, :] == slot) & (own[r : r + 1, :] > 0.5)
        taken = jnp.where(taken, one, zero).astype(jnp.bfloat16)
        found = lax.dot_general(
            js, taken, (((1,), (1,)), ((), ())), preferred_element_type=jnp.float32
        )
        count = jnp.sum(own[r : r + 1, :]).astype(jnp.int32)
        slots = lax.broadcasted_iota(jnp.int32, (1, 40), 1)
        cols = jnp.where(slots < count, 4 * found[:1].astype(jnp.int32) + c, -1)
        cols_ref[r : r + 1, :] = cols[:, :WIDTH]
        starts = starts + jnp.where(row > r, count, 0)
    starts_ref[...] = starts
    map_ref[...] = jnp.zeros((16, BS), jnp.int32)
    for w in range(WIN):
        map_ref[w : w + 1, 0:48] = tab_ref[pl.ds((p0 - HP + w) & (NP - 1), 1), :]
    map_ref[8:16, :] = rank


def square_kernel(map_ref, left_ref, *refs):
    pieces = refs[:WIN]
    out_ref = refs[WIN]
    lefts, rights = refs[WIN + 1 : WIN + 3]
    sums = refs[WIN + 3 : WIN + 3 + PB]
    staged, blank, in_sem, zero_sem, out_sem = refs[WIN + 3 + PB :]
    p0, c = place()
    blank[...] = jnp.zeros(blank.shape, blank.dtype)
    for r in range(PB):
        pltpu.make_async_copy(blank, out_ref.at[r, USED:], zero_sem.at[r]).start()
    copies = [pltpu.make_async_copy(left_ref, lefts, in_sem.at[WIN])]
    core = p0 & 1
    for n in range(WIN):
        w = jnp.where(core == 0, SLOTS[0][n], SLOTS[1][n])
        copies.append(pltpu.make_async_copy(pieces[n], rights.at[w], in_sem.at[n]))
    for copy in copies:
        copy.start()
    for r in range(PB):
        sums[r][...] = jnp.zeros((USED, BS, BS), jnp.float32)
    for copy in copies:
        copy.wait()

    def group_step(g, carry):
        for s0 in range(KG):
            for r in range(PB):
                k = map_ref[HP, 12 * g + KG * r + s0]
                w = (lax.shift_right_logical(k, 2) - p0 + HP) & (WIN - 1)
                kr = k & (PB - 1)
                slots = []
                for s in range(KG):
                    col = map_ref[w, 12 * c + KG * kr + s]
                    slots.append(map_ref[8 + r, lax.shift_right_logical(col, 2)])
                right = jnp.concatenate([rights[w, kr, s] for s in range(KG)], axis=1)
                product = jnp.dot(
                    lefts[g, r, s0], right, preferred_element_type=jnp.float32
                )
                new = [
                    sums[r][slots[s]] + product[:, BS * s : BS * (s + 1)] for s in range(KG)
                ]
                for s in range(KG):
                    sums[r][slots[s]] = new[s]
        return carry

    lax.fori_loop(0, GROUPS, group_step, 0)
    for r in range(PB):
        staged[r] = sums[r][...].astype(jnp.bfloat16)
        pltpu.make_async_copy(staged.at[r], out_ref.at[r, :USED], out_sem.at[r]).start()
    for r in range(PB):
        pltpu.make_async_copy(blank, out_ref.at[r, USED:], zero_sem.at[r]).wait()
        pltpu.make_async_copy(staged.at[r], out_ref.at[r, :USED], out_sem.at[r]).wait()


def indices(table):
    vmem = pl.BlockSpec(memory_space=pltpu.VMEM)
    return pl.pallas_call(
        index_kernel,
        out_shape=(
            jax.ShapeDtypeStruct((PB, WIDTH), jnp.int32),
            jax.ShapeDtypeStruct((PB, 1), jnp.int32),
            jax.ShapeDtypeStruct((16, BS), jnp.int32),
        ),
        in_specs=[vmem],
        out_specs=(vmem, vmem, vmem),
        scratch_shapes=[pltpu.VMEM((PB, NP, BS), jnp.float32)],
        name="indices",
    )(table)


def square(where, left, pieces):
    hbm = pl.BlockSpec(memory_space=pl.ANY)
    return pl.pallas_call(
        square_kernel,
        out_shape=jax.ShapeDtypeStruct((PB, WIDTH, BS, BS), jnp.bfloat16),
        in_specs=[pl.BlockSpec(memory_space=pltpu.SMEM)] + [hbm] * (1 + WIN),
        out_specs=hbm,
        scratch_shapes=[
            pltpu.VMEM((GROUPS, PB, KG, BS, BS), jnp.bfloat16),
            pltpu.VMEM((WIN, PB, KG, BS, BS), jnp.bfloat16),
        ]
        + [pltpu.VMEM((USED, BS, BS), jnp.float32) for _ in range(PB)]
        + [
            pltpu.VMEM((PB, USED, BS, BS), jnp.bfloat16),
            pltpu.VMEM((WIDTH - USED, BS, BS), jnp.bfloat16),
            pltpu.SemaphoreType.DMA((WIN + 1,)),
            pltpu.SemaphoreType.DMA((PB,)),
            pltpu.SemaphoreType.DMA((PB,)),
        ],
        name="square",
    )(where, left, *pieces)


def sent_to_all(shard, axis):
    size = lax.axis_size(axis)
    return lax.all_to_all(
        jnp.broadcast_to(shard[None], (size, *shard.shape)), axis, 0, 0, tiled=True
    )


def moved(block, chips, cross=False, low=None):
    chip_count = NP // 2
    route = []
    for q in range(chip_count):
        for core in range(2):
            step = chips
            if low is not None:
                step = -low if core else low
            route.append((2 * q + core, 2 * ((q + step) % chip_count) + (core ^ cross)))
    return lax.ppermute(block, ROWS, route)


def on_device(blocks, block_cols):
    own = blocks[:, 0]
    slab = sent_to_all(block_cols.reshape(12), ("rows_1", "rows_2", "cols"))
    table = sent_to_all(slab.reshape(8, 48), "rows_0").reshape(NP, 48)
    columns, starts, where = indices(table)
    behind = moved(own, 1)
    ahead = moved(own, -1)
    behind2 = moved(own, 2)
    far = moved(own, 0, True, low=-2)
    left = sent_to_all(own, "cols")
    partner = moved(own, 0, True)
    behind_x = moved(behind, 0, True)
    ahead_x = moved(ahead, 0, True)
    pieces = [own, partner, behind, behind_x, ahead, ahead_x, behind2, far]
    out = square(where, left, pieces)
    return out[:, None], columns[:, None], starts


def solution(mesh):
    split = Mesh(
        mesh.devices.reshape(16, 4, 2, mesh.shape["cols"]), ("rows_0", "rows_1", "rows_2", "cols")
    )
    return jax.shard_map(
        on_device,
        mesh=split,
        in_specs=(P(ROWS, "cols", None, None, None), P(ROWS, "cols", None)),
        out_specs=(P(ROWS, "cols", None, None, None), P(ROWS, "cols", None), P(ROWS, "cols")),
        check_vma=False,
    )
```

```python
import jax
import jax.numpy as jnp
from jax import lax
from jax.experimental import pallas as pl
from jax.experimental.pallas import tpu as pltpu
from jax.sharding import Mesh
from jax.sharding import PartitionSpec as P

HP = 4
PB = 4
KG = 3
GROUPS = 4
BS = 128
NP = 128
WIDTH = 36
USED = 15
WIN = 2 * HP
PER = PB * KG
ROWS = ("rows_0", "rows_1", "rows_2")
SLAB = ("rows_1", "rows_2", "cols")


def place():
    return lax.axis_index(ROWS), lax.axis_index("cols")


def spread_kernel(cols_ref, out_ref):
    _, c = place()
    lane = lax.broadcasted_iota(jnp.int32, (1, BS), 1)
    row = jnp.zeros((1, BS), jnp.int32)
    for r in range(PB):
        for s in range(KG):
            row = jnp.where(lane == PER * c + KG * r + s, cols_ref[r, s], row)
    out_ref[...] = jnp.broadcast_to(row[None], out_ref.shape)


def slab_kernel(in_ref, out_ref):
    rows = []
    for n in range(8):
        part = [in_ref[GROUPS * n + g] for g in range(GROUPS)]
        rows.append((part[0] + part[1]) + (part[2] + part[3]))
    tile = jnp.concatenate(rows, axis=0)
    out_ref[...] = jnp.broadcast_to(tile[None], out_ref.shape)


def bits_set(x):
    x = x - ((x >> 1) & 0x5555)
    x = (x & 0x3333) + ((x >> 2) & 0x3333)
    x = (x + (x >> 4)) & 0x0F0F
    return (x + (x >> 8)) & 0x1F


def index_kernel(tab_ref, cols_ref, starts_ref, map_ref, turned_ref):
    p0, c = place()
    turned_ref[...] = jnp.transpose(tab_ref[...].reshape(NP, BS))
    panel = lax.broadcasted_iota(jnp.int32, (1, NP), 1)
    wants = []
    owns = []
    for r in range(PB):
        want = jnp.zeros((1, NP), jnp.int32)
        for g in range(GROUPS):
            for s in range(KG):
                at = PER * g + KG * r + s
                local = (turned_ref[at : at + 1, :] - PB * (panel - HP)) & (PB * NP - 1)
                want = want | jnp.left_shift(1, local)
        wants.append(want)
        own = jnp.zeros((1, NP), jnp.int32)
        for s in range(KG):
            col = turned_ref[pl.ds(PER * c + KG * r + s, 1), :]
            own = own | jnp.left_shift(1, ((col >> 2) - panel + HP) & (NP - 1))
        owns.append(own)
    pad = [jnp.zeros((PB, NP), jnp.int32)]
    want = jnp.concatenate(wants + pad, axis=0)
    own = jnp.concatenate(owns + pad, axis=0)
    found = jnp.zeros((8, NP), jnp.int32)
    for w in range(WIN):
        there = pltpu.roll(own, (HP - w) % NP, 1) if w != HP else own
        there = there << w
        for kr in range(PB):
            used = -((want >> (PB * w + kr)) & 1)
            found = found | (used & there[kr : kr + 1, :])
    counts = bits_set(found)
    before = jnp.sum(jnp.where(panel < p0, counts, 0).astype(jnp.float32)).astype(jnp.int32)
    here = jnp.where(panel == p0, 1, 0)
    mask = jnp.sum((found * here).astype(jnp.float32), axis=1, keepdims=True)
    count = jnp.sum((counts * here).astype(jnp.float32), axis=1, keepdims=True).astype(jnp.int32)
    mask = mask.astype(jnp.int32)
    lane = lax.broadcasted_iota(jnp.int32, (8, BS), 1)
    held = jnp.where(lane < 16, (jnp.broadcast_to(mask, (8, BS)) >> (lane & 15)) & 1, 0)
    turn = (2 * HP - p0) & (NP - 1)
    turn = jnp.where(turn > 14, 0, turn)
    col_of = lax.broadcasted_iota(jnp.int32, (BS, BS), 1)
    row_of = lax.broadcasted_iota(jnp.int32, (BS, BS), 0)
    ahead = ((row_of - turn) & 15) < ((col_of - turn) & 15)
    ahead = jnp.where(ahead, 1.0, 0.0).astype(jnp.bfloat16)
    rank = jnp.dot(held.astype(jnp.bfloat16), ahead, preferred_element_type=jnp.float32)
    rank = rank.astype(jnp.int32)
    slot = lax.broadcasted_iota(jnp.int32, (40, BS), 0)
    panels = ((p0 - 2 * HP + lane) & (NP - 1)).astype(jnp.bfloat16)
    slots = lax.broadcasted_iota(jnp.int32, (1, 40), 1)
    start = before
    for r in range(PB):
        taken = (rank[r : r + 1, :] == slot) & (held[r : r + 1, :] > 0)
        taken = jnp.where(taken, 1.0, 0.0).astype(jnp.bfloat16)
        col = lax.dot_general(
            panels, taken, (((1,), (1,)), ((), ())), preferred_element_type=jnp.float32
        )
        cols = jnp.where(slots < count[r : r + 1, :], PB * col[:1].astype(jnp.int32) + c, -1)
        cols_ref[r : r + 1, :] = cols[:, :WIDTH]
        starts_ref[r : r + 1, :] = jnp.broadcast_to(start, (1, 1))
        start = start + count[r : r + 1, :]
    for w in range(WIN):
        at = (p0 - HP + w) & (NP - 1)
        row = tab_ref[at >> 3, pl.ds(at & 7, 1), :]
        map_ref[w : w + 1, :] = (((row >> 2) - at + HP) & (NP - 1)) + w
        if w == HP:
            map_ref[WIN : WIN + 1, :] = (row - PB * (p0 - HP)) & (PB * NP - 1)
    map_ref[WIN + 1 : 16, :] = rank[: 16 - WIN - 1, :]


def square_kernel(map_ref, left_ref, pair_ref, next_ref, swap_ref, far_ref, last_ref, *refs):
    out_ref = refs[0]
    lefts, rights = refs[1:3]
    sums = refs[3 : 3 + PB]
    staged, blank, in_sem, zero_sem, out_sem = refs[3 + PB :]
    p0, c = place()
    core = p0 & 1
    blank[...] = jnp.zeros(blank.shape, blank.dtype)
    for r in range(PB):
        pltpu.make_async_copy(blank, out_ref.at[r, USED:], zero_sem.at[r]).start()
    moves = (
        (pair_ref, 0, HP, HP),
        (pair_ref, 1, 5, 3),
        (next_ref, 0, 2, 6),
        (next_ref, 1, 3, 5),
        (swap_ref, 0, 7, 1),
        (swap_ref, 1, 6, 2),
        (far_ref, 1, 1, 7),
    )
    copies = [pltpu.make_async_copy(left_ref, lefts, in_sem.at[WIN])]
    for n, (ref, half, even, odd) in enumerate(moves):
        w = jnp.where(core == 0, even, odd)
        copies.append(pltpu.make_async_copy(ref.at[half], rights.at[w], in_sem.at[n]))
    for copy in copies:
        copy.start()
    low = pltpu.make_async_copy(far_ref.at[0], rights.at[0], in_sem.at[WIN - 1])
    crossed = pltpu.make_async_copy(last_ref, rights.at[0], in_sem.at[WIN - 1])
    pl.when(core == 0)(low.start)
    pl.when(core == 1)(crossed.start)
    for r in range(PB):
        sums[r][...] = jnp.zeros((USED, BS, BS), jnp.float32)
    for copy in copies:
        copy.wait()
    low.wait()

    def group_step(g, carry):
        for s0 in range(KG):
            for r in range(PB):
                local = map_ref[WIN, PER * g + KG * r + s0]
                w = local >> 2
                kr = local & (PB - 1)
                slots = []
                for s in range(KG):
                    slots.append(map_ref[WIN + 1 + r, map_ref[w, PER * c + KG * kr + s]])
                right = jnp.concatenate([rights[w, kr, s] for s in range(KG)], axis=1)
                product = jnp.dot(lefts[g, r, s0], right, preferred_element_type=jnp.float32)
                new = [
                    sums[r][slots[s]] + product[:, BS * s : BS * (s + 1)] for s in range(KG)
                ]
                for s in range(KG):
                    sums[r][slots[s]] = new[s]
        return carry

    lax.fori_loop(0, GROUPS, group_step, 0)
    for r in range(PB):
        staged[r] = sums[r][...].astype(jnp.bfloat16)
        pltpu.make_async_copy(staged.at[r], out_ref.at[r, :USED], out_sem.at[r]).start()
    for r in range(PB):
        pltpu.make_async_copy(blank, out_ref.at[r, USED:], zero_sem.at[r]).wait()
        pltpu.make_async_copy(staged.at[r], out_ref.at[r, :USED], out_sem.at[r]).wait()


VMEM = pl.BlockSpec(memory_space=pltpu.VMEM)
SMEM = pl.BlockSpec(memory_space=pltpu.SMEM)
HBM = pl.BlockSpec(memory_space=pl.ANY)


def spread(cols):
    return pl.pallas_call(
        spread_kernel,
        out_shape=jax.ShapeDtypeStruct((32, 1, BS), jnp.int32),
        in_specs=[SMEM],
        out_specs=VMEM,
        name="spread",
    )(cols)


def slab_table(parts):
    return pl.pallas_call(
        slab_kernel,
        out_shape=jax.ShapeDtypeStruct((16, 8, BS), jnp.int32),
        in_specs=[VMEM],
        out_specs=VMEM,
        name="slab_table",
    )(parts)


def indices(table):
    return pl.pallas_call(
        index_kernel,
        out_shape=(
            jax.ShapeDtypeStruct((PB, WIDTH), jnp.int32),
            jax.ShapeDtypeStruct((PB, 1), jnp.int32),
            jax.ShapeDtypeStruct((16, BS), jnp.int32),
        ),
        in_specs=[VMEM],
        out_specs=(VMEM, VMEM, VMEM),
        scratch_shapes=[pltpu.VMEM((BS, NP), jnp.int32)],
        name="indices",
    )(table)


def square(where, left, pieces):
    return pl.pallas_call(
        square_kernel,
        out_shape=jax.ShapeDtypeStruct((PB, WIDTH, BS, BS), jnp.bfloat16),
        in_specs=[SMEM] + [HBM] * (1 + len(pieces)),
        out_specs=HBM,
        scratch_shapes=[
            pltpu.VMEM((GROUPS, PB, KG, BS, BS), jnp.bfloat16),
            pltpu.VMEM((WIN, PB, KG, BS, BS), jnp.bfloat16),
        ]
        + [pltpu.VMEM((USED, BS, BS), jnp.float32) for _ in range(PB)]
        + [
            pltpu.VMEM((PB, USED, BS, BS), jnp.bfloat16),
            pltpu.VMEM((WIDTH - USED, BS, BS), jnp.bfloat16),
            pltpu.SemaphoreType.DMA((WIN + 1,)),
            pltpu.SemaphoreType.DMA((PB,)),
            pltpu.SemaphoreType.DMA((PB,)),
        ],
        name="square",
    )(where, left, *pieces)


def exchange(array, axes):
    return lax.all_to_all(array, axes, 0, 0, tiled=True)


def swapped(block):
    return lax.ppermute(block, "rows_2", [(0, 1), (1, 0)])


def outward(pair):
    chips = NP // 2
    route = []
    for q in range(chips):
        route.append((2 * q, 2 * ((q + 1) % chips)))
        route.append((2 * q + 1, 2 * ((q - 1) % chips) + 1))
    return lax.ppermute(pair, ROWS, route)


def on_device(blocks, block_cols):
    own = blocks[:, 0]
    parts = exchange(spread(block_cols[:, 0]), SLAB)
    table = exchange(slab_table(parts), "rows_0")
    columns, starts, where = indices(table)
    partner = swapped(own)
    pair = jnp.stack([own, partner])
    near = outward(pair)
    left = exchange(jnp.broadcast_to(own[None], (GROUPS, *own.shape)), "cols")
    far = outward(near)
    swap = swapped(near)
    last = lax.ppermute(far[1], "rows_2", [(0, 1)])
    out = square(where, left, (pair, near, swap, far, last))
    return out[:, None], columns[:, None], starts


def solution(mesh):
    split = Mesh(
        mesh.devices.reshape(16, 4, 2, mesh.shape["cols"]), ("rows_0", "rows_1", "rows_2", "cols")
    )
    return jax.shard_map(
        on_device,
        mesh=split,
        in_specs=(P(ROWS, "cols", None, None, None), P(ROWS, "cols", None)),
        out_specs=(P(ROWS, "cols", None, None, None), P(ROWS, "cols", None), P(ROWS, "cols")),
        check_vma=False,
    )
```

```python
import jax
import jax.numpy as jnp
from jax import lax
from jax.experimental import pallas as pl
from jax.experimental.pallas import tpu as pltpu
from jax.sharding import Mesh
from jax.sharding import PartitionSpec as P

HP = 4
PB = 4
KG = 3
GROUPS = 4
BS = 128
NP = 128
WIDTH = 36
USED = 15
WIN = 2 * HP
PER = PB * KG
ROWS = ("rows_0", "rows_1", "rows_2")
SLAB = ("rows_1", "rows_2", "cols")


def place():
    return lax.axis_index(ROWS), lax.axis_index("cols")


def spread_kernel(cols_ref, out_ref):
    _, c = place()
    lane = lax.broadcasted_iota(jnp.int32, (1, BS), 1)
    row = jnp.zeros((1, BS), jnp.int32)
    for r in range(PB):
        for s in range(KG):
            row = jnp.where(lane == PER * c + KG * r + s, cols_ref[r, s], row)
    out_ref[...] = jnp.broadcast_to(row[None], out_ref.shape)


def slab_kernel(in_ref, out_ref):
    rows = []
    for n in range(8):
        part = [in_ref[GROUPS * n + g] for g in range(GROUPS)]
        rows.append((part[0] + part[1]) + (part[2] + part[3]))
    tile = jnp.concatenate(rows, axis=0)
    out_ref[...] = jnp.broadcast_to(tile[None], out_ref.shape)


def bits_set(x):
    x = x - ((x >> 1) & 0x5555)
    x = (x & 0x3333) + ((x >> 2) & 0x3333)
    x = (x + (x >> 4)) & 0x0F0F
    return (x + (x >> 8)) & 0x1F


def index_kernel(tab_ref, cols_ref, starts_ref, map_ref, turned_ref):
    p0, c = place()
    turned_ref[...] = jnp.transpose(tab_ref[...].reshape(NP, BS))
    panel = lax.broadcasted_iota(jnp.int32, (1, NP), 1)
    wants = []
    owns = []
    for r in range(PB):
        want = jnp.zeros((1, NP), jnp.int32)
        for g in range(GROUPS):
            for s in range(KG):
                at = PER * g + KG * r + s
                local = (turned_ref[at : at + 1, :] - PB * (panel - HP)) & (PB * NP - 1)
                want = want | jnp.left_shift(1, local)
        wants.append(want)
        own = jnp.zeros((1, NP), jnp.int32)
        for s in range(KG):
            col = turned_ref[pl.ds(PER * c + KG * r + s, 1), :]
            own = own | jnp.left_shift(1, ((col >> 2) - panel + HP) & (NP - 1))
        owns.append(own)
    pad = [jnp.zeros((PB, NP), jnp.int32)]
    want = jnp.concatenate(wants + pad, axis=0)
    own = jnp.concatenate(owns + pad, axis=0)
    found = jnp.zeros((8, NP), jnp.int32)
    for w in range(WIN):
        there = pltpu.roll(own, (HP - w) % NP, 1) if w != HP else own
        there = there << w
        for kr in range(PB):
            used = -((want >> (PB * w + kr)) & 1)
            found = found | (used & there[kr : kr + 1, :])
    counts = bits_set(found)
    before = jnp.sum(jnp.where(panel < p0, counts, 0).astype(jnp.float32)).astype(jnp.int32)
    here = jnp.where(panel == p0, 1, 0)
    mask = jnp.sum((found * here).astype(jnp.float32), axis=1, keepdims=True)
    count = jnp.sum((counts * here).astype(jnp.float32), axis=1, keepdims=True).astype(jnp.int32)
    mask = mask.astype(jnp.int32)
    lane = lax.broadcasted_iota(jnp.int32, (8, BS), 1)
    held = jnp.where(lane < 16, (jnp.broadcast_to(mask, (8, BS)) >> (lane & 15)) & 1, 0)
    turn = (2 * HP - p0) & (NP - 1)
    turn = jnp.where(turn > 14, 0, turn)
    col_of = lax.broadcasted_iota(jnp.int32, (BS, BS), 1)
    row_of = lax.broadcasted_iota(jnp.int32, (BS, BS), 0)
    ahead = ((row_of - turn) & 15) < ((col_of - turn) & 15)
    ahead = jnp.where(ahead, 1.0, 0.0).astype(jnp.bfloat16)
    rank = jnp.dot(held.astype(jnp.bfloat16), ahead, preferred_element_type=jnp.float32)
    rank = rank.astype(jnp.int32)
    slot = lax.broadcasted_iota(jnp.int32, (40, BS), 0)
    panels = ((p0 - 2 * HP + lane) & (NP - 1)).astype(jnp.bfloat16)
    slots = lax.broadcasted_iota(jnp.int32, (1, 40), 1)
    start = before
    for r in range(PB):
        taken = (rank[r : r + 1, :] == slot) & (held[r : r + 1, :] > 0)
        taken = jnp.where(taken, 1.0, 0.0).astype(jnp.bfloat16)
        col = lax.dot_general(
            panels, taken, (((1,), (1,)), ((), ())), preferred_element_type=jnp.float32
        )
        cols = jnp.where(slots < count[r : r + 1, :], PB * col[:1].astype(jnp.int32) + c, -1)
        cols_ref[r : r + 1, :] = cols[:, :WIDTH]
        starts_ref[:, r : r + 1] = jnp.broadcast_to(start, (1, 1))
        start = start + count[r : r + 1, :]
    for w in range(WIN):
        at = (p0 - HP + w) & (NP - 1)
        row = tab_ref[at >> 3, pl.ds(at & 7, 1), :]
        map_ref[w : w + 1, :] = (((row >> 2) - at + HP) & (NP - 1)) + w
        if w == HP:
            map_ref[WIN : WIN + 1, :] = (row - PB * (p0 - HP)) & (PB * NP - 1)
    map_ref[WIN + 1 : 16, :] = rank[: 16 - WIN - 1, :]


def square_kernel(map_ref, up_ref, over_ref, down_ref, pair_ref, next_ref, swap_ref, far_ref, last_ref, *refs):
    out_ref = refs[0]
    rights = refs[1]
    sums = refs[2 : 2 + PB]
    staged, blank, in_sem, zero_sem, out_sem = refs[2 + PB :]
    p0, c = place()
    core = p0 & 1
    blank[...] = jnp.zeros(blank.shape, blank.dtype)
    for r in range(PB):
        pltpu.make_async_copy(blank, out_ref.at[r, USED:], zero_sem.at[r]).start()
    moves = (
        (pair_ref, 0, HP, HP),
        (pair_ref, 1, 5, 3),
        (next_ref, 0, 2, 6),
        (next_ref, 1, 3, 5),
        (swap_ref, 0, 7, 1),
        (swap_ref, 1, 6, 2),
        (far_ref, 1, 1, 7),
    )
    copies = []
    for n, (ref, half, even, odd) in enumerate(moves):
        w = jnp.where(core == 0, even, odd)
        copies.append(pltpu.make_async_copy(ref.at[half], rights.at[w], in_sem.at[n]))
    for copy in copies:
        copy.start()
    low = pltpu.make_async_copy(far_ref.at[0], rights.at[0], in_sem.at[WIN - 1])
    crossed = pltpu.make_async_copy(last_ref, rights.at[0], in_sem.at[WIN - 1])
    pl.when(core == 0)(low.start)
    pl.when(core == 1)(crossed.start)
    for r in range(PB):
        sums[r][...] = jnp.zeros((USED, BS, BS), jnp.float32)
    for copy in copies:
        copy.wait()
    low.wait()

    def block_step(s0, carry):
        for d in range(GROUPS):
            g = (c + d) & (GROUPS - 1)
            left_ref = (None, up_ref, over_ref, down_ref)[d]
            for r in range(PB):
                local = map_ref[WIN, PER * g + KG * r + s0]
                w = local >> 2
                kr = local & (PB - 1)
                slots = []
                for s in range(KG):
                    slots.append(map_ref[WIN + 1 + r, map_ref[w, PER * c + KG * kr + s]])
                right = jnp.concatenate([rights[w, kr, s] for s in range(KG)], axis=1)
                left = left_ref[r, s0] if d else pair_ref[0, r, s0]
                product = jnp.dot(left, right, preferred_element_type=jnp.float32)
                new = [
                    sums[r][slots[s]] + product[:, BS * s : BS * (s + 1)] for s in range(KG)
                ]
                for s in range(KG):
                    sums[r][slots[s]] = new[s]
        return carry

    lax.fori_loop(0, KG, block_step, 0)
    for r in range(PB):
        staged[r] = sums[r][...].astype(jnp.bfloat16)
        pltpu.make_async_copy(staged.at[r], out_ref.at[r, :USED], out_sem.at[r]).start()
    for r in range(PB):
        pltpu.make_async_copy(blank, out_ref.at[r, USED:], zero_sem.at[r]).wait()
        pltpu.make_async_copy(staged.at[r], out_ref.at[r, :USED], out_sem.at[r]).wait()


VMEM = pl.BlockSpec(memory_space=pltpu.VMEM)
SMEM = pl.BlockSpec(memory_space=pltpu.SMEM)
HBM = pl.BlockSpec(memory_space=pl.ANY)


def near_core(array):
    return pltpu.with_memory_space_constraint(array, pltpu.VMEM)


def spread(cols):
    return pl.pallas_call(
        spread_kernel,
        out_shape=jax.ShapeDtypeStruct((32, 1, BS), jnp.int32),
        in_specs=[SMEM],
        out_specs=VMEM,
        compiler_params=pltpu.CompilerParams(vmem_limit_bytes=8 << 20),
        name="spread",
    )(cols)


def slab_table(parts):
    return pl.pallas_call(
        slab_kernel,
        out_shape=jax.ShapeDtypeStruct((16, 8, BS), jnp.int32),
        in_specs=[VMEM],
        out_specs=VMEM,
        compiler_params=pltpu.CompilerParams(vmem_limit_bytes=8 << 20),
        name="slab_table",
    )(parts)


def indices(table):
    return pl.pallas_call(
        index_kernel,
        out_shape=(
            jax.ShapeDtypeStruct((PB, WIDTH), jnp.int32),
            jax.ShapeDtypeStruct((1, PB), jnp.int32),
            jax.ShapeDtypeStruct((16, BS), jnp.int32),
        ),
        in_specs=[VMEM],
        out_specs=(VMEM, VMEM, VMEM),
        scratch_shapes=[pltpu.VMEM((BS, NP), jnp.int32)],
        compiler_params=pltpu.CompilerParams(vmem_limit_bytes=8 << 20),
        name="indices",
    )(table)


def square(where, lefts, pieces):
    return pl.pallas_call(
        square_kernel,
        out_shape=jax.ShapeDtypeStruct((PB, WIDTH, BS, BS), jnp.bfloat16),
        in_specs=[SMEM] + [VMEM] * (len(lefts) + len(pieces)),
        out_specs=HBM,
        scratch_shapes=[
            pltpu.VMEM((WIN, PB, KG, BS, BS), jnp.bfloat16),
        ]
        + [pltpu.VMEM((USED, BS, BS), jnp.float32) for _ in range(PB)]
        + [
            pltpu.VMEM((PB, USED, BS, BS), jnp.bfloat16),
            pltpu.VMEM((WIDTH - USED, BS, BS), jnp.bfloat16),
            pltpu.SemaphoreType.DMA((WIN,)),
            pltpu.SemaphoreType.DMA((PB,)),
            pltpu.SemaphoreType.DMA((PB,)),
        ],
        compiler_params=pltpu.CompilerParams(vmem_limit_bytes=24 << 20),
        name="square",
    )(where, *[near_core(piece) for piece in (*lefts, *pieces)])


def exchange(array, axes):
    return lax.all_to_all(array, axes, 0, 0, tiled=True)


def swapped(block):
    return lax.ppermute(block, "rows_2", [(0, 1), (1, 0)])


def turned(block, distance):
    return lax.ppermute(block, "cols", [((c + distance) % GROUPS, c) for c in range(GROUPS)])


def outward(pair):
    chips = NP // 2
    route = []
    for q in range(chips):
        route.append((2 * q, 2 * ((q + 1) % chips)))
        route.append((2 * q + 1, 2 * ((q - 1) % chips) + 1))
    return lax.ppermute(pair, ROWS, route)


def on_device(blocks, block_cols):
    own = blocks[:, 0]
    parts = exchange(spread(block_cols[:, 0]), SLAB)
    table = exchange(slab_table(parts), "rows_0")
    columns, starts, where = indices(table)
    partner = swapped(own)
    pair = jnp.stack([own, partner])
    near = outward(pair)
    up = turned(own, 1)
    down = turned(own, 3)
    over = turned(own, 2)
    far = outward(near)
    swap = swapped(near)
    last = lax.ppermute(far[1], "rows_2", [(0, 1)])
    out = square(where, (up, over, down), (pair, near, swap, far, last))
    return out[:, None], columns[:, None], starts.reshape(PB, 1)


def solution(mesh):
    split = Mesh(
        mesh.devices.reshape(16, 4, 2, mesh.shape["cols"]), ("rows_0", "rows_1", "rows_2", "cols")
    )
    return jax.shard_map(
        on_device,
        mesh=split,
        in_specs=(P(ROWS, "cols", None, None, None), P(ROWS, "cols", None)),
        out_specs=(P(ROWS, "cols", None, None, None), P(ROWS, "cols", None), P(ROWS, "cols")),
        check_vma=False,
    )
```

```python
import jax
import jax.numpy as jnp
from jax import lax
from jax.experimental import pallas as pl
from jax.experimental.pallas import tpu as pltpu
from jax.sharding import Mesh
from jax.sharding import PartitionSpec as P

HP = 4
PB = 4
KG = 3
GROUPS = 4
BS = 128
NP = 128
WIDTH = 36
USED = 15
WIN = 2 * HP
PER = PB * KG
ROWS = ("rows_0", "rows_1", "rows_2")
CHIP_LINE = ("rows_2", "cols")
CHIPS = ("rows_0", "rows_1")
HALF = 64


def place():
    return lax.axis_index(ROWS), lax.axis_index("cols")


def spread_kernel(cols_ref, out_ref):
    p0, c = place()
    lane = lax.broadcasted_iota(jnp.int32, (1, BS), 1)
    first = HALF * (p0 & 1) + PER * c
    row = jnp.zeros((1, BS), jnp.int32)
    for r in range(PB):
        for s in range(KG):
            row = jnp.where(lane == first + KG * r + s, cols_ref[r, s] >> 2, row)
    out_ref[...] = jnp.broadcast_to(row[None], out_ref.shape)


def chip_kernel(in_ref, out_ref):
    part = [in_ref[n] for n in range(2 * GROUPS)]
    while len(part) > 1:
        part = [a + b for a, b in zip(part[::2], part[1::2])]
    out_ref[...] = jnp.broadcast_to(part[0][None], out_ref.shape)


def bits_set(x):
    x = x - ((x >> 1) & 0x5555)
    x = (x & 0x3333) + ((x >> 2) & 0x3333)
    x = (x + (x >> 4)) & 0x0F0F
    return (x + (x >> 8)) & 0x1F


def index_kernel(tab_ref, cols_ref, starts_ref, map_ref, table_ref, turned_ref):
    p0, c = place()
    for n in range(HALF):
        table_ref[n : n + 1, :] = tab_ref[n]
    table = table_ref[...].astype(jnp.float32).astype(jnp.bfloat16)
    chip = lax.broadcasted_iota(jnp.int32, (HALF, NP), 0)
    spot = lax.broadcasted_iota(jnp.int32, (HALF, NP), 1)
    turned = jnp.zeros((HALF, NP), jnp.float32)
    for core in range(2):
        pick = jnp.where(spot == 2 * chip + core, 1.0, 0.0).astype(jnp.bfloat16)
        turned = turned + lax.dot_general(
            table[:, HALF * core : HALF * (core + 1)],
            pick,
            (((0,), (0,)), ((), ())),
            preferred_element_type=jnp.float32,
        )
    turned_ref[...] = (turned.astype(jnp.int32) - spot + HP) & (NP - 1)
    panel = lax.broadcasted_iota(jnp.int32, (1, NP), 1)
    wants = []
    owns = []
    for r in range(PB):
        want = jnp.zeros((1, NP), jnp.int32)
        for g in range(GROUPS):
            for s in range(KG):
                at = PER * g + KG * r + s
                want = want | jnp.left_shift(1, PB * turned_ref[at : at + 1, :] + g)
        wants.append(want)
        own = jnp.zeros((1, NP), jnp.int32)
        for s in range(KG):
            own = own | jnp.left_shift(1, turned_ref[pl.ds(PER * c + KG * r + s, 1), :])
        owns.append(own)
    pad = [jnp.zeros((PB, NP), jnp.int32)]
    want = jnp.concatenate(wants + pad, axis=0)
    own = jnp.concatenate(owns + pad, axis=0)
    found = jnp.zeros((8, NP), jnp.int32)
    for w in range(WIN):
        there = pltpu.roll(own, (HP - w) % NP, 1) if w != HP else own
        there = there << w
        for kr in range(PB):
            used = -((want >> (PB * w + kr)) & 1)
            found = found | (used & there[kr : kr + 1, :])
    counts = bits_set(found)
    before = jnp.sum(jnp.where(panel < p0, counts, 0).astype(jnp.float32)).astype(jnp.int32)
    here = jnp.where(panel == p0, 1, 0)
    mask = jnp.sum((found * here).astype(jnp.float32), axis=1, keepdims=True)
    count = jnp.sum((counts * here).astype(jnp.float32), axis=1, keepdims=True).astype(jnp.int32)
    mask = mask.astype(jnp.int32)
    lane = lax.broadcasted_iota(jnp.int32, (8, BS), 1)
    held = jnp.where(lane < 16, (jnp.broadcast_to(mask, (8, BS)) >> (lane & 15)) & 1, 0)
    turn = (2 * HP - p0) & (NP - 1)
    turn = jnp.where(turn > 14, 0, turn)
    col_of = lax.broadcasted_iota(jnp.int32, (BS, BS), 1)
    row_of = lax.broadcasted_iota(jnp.int32, (BS, BS), 0)
    ahead = ((row_of - turn) & 15) < ((col_of - turn) & 15)
    ahead = jnp.where(ahead, 1.0, 0.0).astype(jnp.bfloat16)
    rank = jnp.dot(held.astype(jnp.bfloat16), ahead, preferred_element_type=jnp.float32)
    rank = rank.astype(jnp.int32)
    slot = lax.broadcasted_iota(jnp.int32, (40, BS), 0)
    panels = ((p0 - 2 * HP + lane) & (NP - 1)).astype(jnp.bfloat16)
    slots = lax.broadcasted_iota(jnp.int32, (1, 40), 1)
    start = before
    for r in range(PB):
        taken = (rank[r : r + 1, :] == slot) & (held[r : r + 1, :] > 0)
        taken = jnp.where(taken, 1.0, 0.0).astype(jnp.bfloat16)
        col = lax.dot_general(
            panels, taken, (((1,), (1,)), ((), ())), preferred_element_type=jnp.float32
        )
        cols = jnp.where(slots < count[r : r + 1, :], PB * col[:1].astype(jnp.int32) + c, -1)
        cols_ref[r : r + 1, :] = cols[:, :WIDTH]
        starts_ref[:, r : r + 1] = jnp.broadcast_to(start, (1, 1))
        start = start + count[r : r + 1, :]
    spread = lax.broadcasted_iota(jnp.int32, (1, BS), 1)
    group = jnp.zeros((1, BS), jnp.int32)
    for g in range(1, GROUPS):
        group = group + jnp.where(spread >= PER * g, 1, 0)
    for w in range(WIN):
        at = (p0 - HP + w) & (NP - 1)
        row = table_ref[pl.ds(at >> 1, 1), :]
        row = jnp.where((at & 1) == 1, pltpu.roll(row, HALF, 1), row)
        row = (row - at + HP) & (NP - 1)
        map_ref[w : w + 1, :] = row + w
        if w == HP:
            map_ref[WIN : WIN + 1, :] = PB * row + group
    map_ref[WIN + 1 : 16, :] = rank[: 16 - WIN - 1, :]


def square_kernel(map_ref, up_ref, over_ref, down_ref, pair_ref, next_ref, swap_ref, far_ref, last_ref, *refs):
    out_ref = refs[0]
    rights = refs[1]
    sums = refs[2 : 2 + PB]
    staged, blank, in_sem, zero_sem, out_sem = refs[2 + PB :]
    p0, c = place()
    core = p0 & 1
    blank[...] = jnp.zeros(blank.shape, blank.dtype)
    for r in range(PB):
        pltpu.make_async_copy(blank, out_ref.at[r, USED:], zero_sem.at[r]).start()
    moves = (
        (pair_ref, 0, HP, HP),
        (pair_ref, 1, 5, 3),
        (next_ref, 0, 2, 6),
        (next_ref, 1, 3, 5),
        (swap_ref, 0, 7, 1),
        (swap_ref, 1, 6, 2),
        (far_ref, 1, 1, 7),
    )
    copies = []
    for n, (ref, half, even, odd) in enumerate(moves):
        w = jnp.where(core == 0, even, odd)
        copies.append(pltpu.make_async_copy(ref.at[half], rights.at[w], in_sem.at[n]))
    for copy in copies:
        copy.start()
    low = pltpu.make_async_copy(far_ref.at[0], rights.at[0], in_sem.at[WIN - 1])
    crossed = pltpu.make_async_copy(last_ref, rights.at[0], in_sem.at[WIN - 1])
    pl.when(core == 0)(low.start)
    pl.when(core == 1)(crossed.start)
    for r in range(PB):
        sums[r][...] = jnp.zeros((USED, BS, BS), jnp.float32)
    for copy in copies:
        copy.wait()
    low.wait()

    def block_step(s0, carry):
        for d in range(GROUPS):
            g = (c + d) & (GROUPS - 1)
            left_ref = (None, up_ref, over_ref, down_ref)[d]
            for r in range(PB):
                local = map_ref[WIN, PER * g + KG * r + s0]
                w = local >> 2
                kr = local & (PB - 1)
                slots = []
                for s in range(KG):
                    slots.append(map_ref[WIN + 1 + r, map_ref[w, PER * c + KG * kr + s]])
                right = jnp.concatenate([rights[w, kr, s] for s in range(KG)], axis=1)
                left = left_ref[r, s0] if d else pair_ref[0, r, s0]
                product = jnp.dot(left, right, preferred_element_type=jnp.float32)
                new = [
                    sums[r][slots[s]] + product[:, BS * s : BS * (s + 1)] for s in range(KG)
                ]
                for s in range(KG):
                    sums[r][slots[s]] = new[s]
        return carry

    lax.fori_loop(0, KG, block_step, 0)
    for r in range(PB):
        staged[r] = sums[r][...].astype(jnp.bfloat16)
        pltpu.make_async_copy(staged.at[r], out_ref.at[r, :USED], out_sem.at[r]).start()
    for r in range(PB):
        pltpu.make_async_copy(blank, out_ref.at[r, USED:], zero_sem.at[r]).wait()
        pltpu.make_async_copy(staged.at[r], out_ref.at[r, :USED], out_sem.at[r]).wait()


VMEM = pl.BlockSpec(memory_space=pltpu.VMEM)
SMEM = pl.BlockSpec(memory_space=pltpu.SMEM)
HBM = pl.BlockSpec(memory_space=pl.ANY)


def near_core(array):
    return pltpu.with_memory_space_constraint(array, pltpu.VMEM)


def spread(cols):
    return pl.pallas_call(
        spread_kernel,
        out_shape=jax.ShapeDtypeStruct((2 * GROUPS, 1, BS), jnp.int32),
        in_specs=[SMEM],
        out_specs=VMEM,
        compiler_params=pltpu.CompilerParams(vmem_limit_bytes=8 << 20),
        name="spread",
    )(cols)


def chip_table(parts):
    return pl.pallas_call(
        chip_kernel,
        out_shape=jax.ShapeDtypeStruct((HALF, 1, BS), jnp.int32),
        in_specs=[VMEM],
        out_specs=VMEM,
        compiler_params=pltpu.CompilerParams(vmem_limit_bytes=8 << 20),
        name="chip_table",
    )(parts)


def indices(table):
    return pl.pallas_call(
        index_kernel,
        out_shape=(
            jax.ShapeDtypeStruct((PB, WIDTH), jnp.int32),
            jax.ShapeDtypeStruct((1, PB), jnp.int32),
            jax.ShapeDtypeStruct((16, BS), jnp.int32),
        ),
        in_specs=[VMEM],
        out_specs=(VMEM, VMEM, VMEM),
        scratch_shapes=[pltpu.VMEM((HALF, BS), jnp.int32), pltpu.VMEM((HALF, NP), jnp.int32)],
        compiler_params=pltpu.CompilerParams(vmem_limit_bytes=8 << 20),
        name="indices",
    )(table)


def square(where, lefts, pieces):
    return pl.pallas_call(
        square_kernel,
        out_shape=jax.ShapeDtypeStruct((PB, WIDTH, BS, BS), jnp.bfloat16),
        in_specs=[SMEM] + [VMEM] * (len(lefts) + len(pieces)),
        out_specs=HBM,
        scratch_shapes=[
            pltpu.VMEM((WIN, PB, KG, BS, BS), jnp.bfloat16),
        ]
        + [pltpu.VMEM((USED, BS, BS), jnp.float32) for _ in range(PB)]
        + [
            pltpu.VMEM((PB, USED, BS, BS), jnp.bfloat16),
            pltpu.VMEM((WIDTH - USED, BS, BS), jnp.bfloat16),
            pltpu.SemaphoreType.DMA((WIN,)),
            pltpu.SemaphoreType.DMA((PB,)),
            pltpu.SemaphoreType.DMA((PB,)),
        ],
        compiler_params=pltpu.CompilerParams(vmem_limit_bytes=24 << 20),
        name="square",
    )(where, *[near_core(piece) for piece in (*lefts, *pieces)])


def exchange(array, axes):
    return lax.all_to_all(array, axes, 0, 0, tiled=True)


def swapped(block):
    return lax.ppermute(block, "rows_2", [(0, 1), (1, 0)])


def turned(block, distance):
    return lax.ppermute(block, "cols", [((c + distance) % GROUPS, c) for c in range(GROUPS)])


def outward(pair):
    chips = NP // 2
    route = []
    for q in range(chips):
        route.append((2 * q, 2 * ((q + 1) % chips)))
        route.append((2 * q + 1, 2 * ((q - 1) % chips) + 1))
    return lax.ppermute(pair, ROWS, route)


def on_device(blocks, block_cols):
    own = blocks[:, 0]
    parts = exchange(spread(block_cols[:, 0]), CHIP_LINE)
    table = exchange(chip_table(parts), CHIPS)
    columns, starts, where = indices(table)
    partner = swapped(own)
    pair = jnp.stack([own, partner])
    near = outward(pair)
    up = turned(own, 1)
    down = turned(own, 3)
    over = turned(own, 2)
    far = outward(near)
    swap = swapped(near)
    last = lax.ppermute(far[1], "rows_2", [(0, 1)])
    out = square(where, (up, over, down), (pair, near, swap, far, last))
    return out[:, None], columns[:, None], starts.reshape(PB, 1)


def solution(mesh):
    split = Mesh(
        mesh.devices.reshape(16, 4, 2, mesh.shape["cols"]), ("rows_0", "rows_1", "rows_2", "cols")
    )
    return jax.shard_map(
        on_device,
        mesh=split,
        in_specs=(P(ROWS, "cols", None, None, None), P(ROWS, "cols", None)),
        out_specs=(P(ROWS, "cols", None, None, None), P(ROWS, "cols", None), P(ROWS, "cols")),
        check_vma=False,
    )
```

```python
import jax
import jax.numpy as jnp
from jax import lax
from jax.experimental import pallas as pl
from jax.experimental.pallas import tpu as pltpu
from jax.sharding import Mesh
from jax.sharding import PartitionSpec as P

HP = 4
PB = 4
KG = 3
GROUPS = 4
BS = 128
NP = 128
WIDTH = 36
USED = 15
WIN = 2 * HP
ROWS = ("rows_0", "rows_1", "rows_2")
ROOM = 16


def place():
    return lax.axis_index(ROWS), lax.axis_index("cols")


def spread_kernel(cols_ref, out_ref):
    lane = lax.broadcasted_iota(jnp.int32, (1, BS), 1)
    row = jnp.zeros((1, BS), jnp.int32)
    for r in range(PB):
        for s in range(KG):
            row = jnp.where(lane == KG * r + s, cols_ref[r, s] >> 2, row)
    out_ref[...] = jnp.broadcast_to(row[None], out_ref.shape)


def turn_kernel(in_ref, out_ref, table_ref):
    for n in range(NP):
        table_ref[n : n + 1, :] = in_ref[n]
    turned = jnp.transpose(table_ref[...])
    out_ref[...] = jnp.broadcast_to(turned[None, :ROOM], out_ref.shape)


def bits_set(x):
    x = x - ((x >> 1) & 0x5555)
    x = (x & 0x3333) + ((x >> 2) & 0x3333)
    x = (x + (x >> 4)) & 0x0F0F
    return (x + (x >> 8)) & 0x1F


def index_kernel(tab_ref, cols_ref, starts_ref, map_ref, turned_ref):
    p0, c = place()
    spot = lax.broadcasted_iota(jnp.int32, (GROUPS * ROOM, NP), 1)
    turned = (tab_ref[...].reshape(GROUPS * ROOM, NP) - spot + HP) & (NP - 1)
    turned_ref[...] = turned
    panel = lax.broadcasted_iota(jnp.int32, (1, NP), 1)
    wants = []
    owns = []
    for r in range(PB):
        want = jnp.zeros((1, NP), jnp.int32)
        for g in range(GROUPS):
            for s in range(KG):
                at = ROOM * g + KG * r + s
                want = want | jnp.left_shift(1, PB * turned_ref[at : at + 1, :] + g)
        wants.append(want)
        own = jnp.zeros((1, NP), jnp.int32)
        for s in range(KG):
            own = own | jnp.left_shift(1, turned_ref[pl.ds(ROOM * c + KG * r + s, 1), :])
        owns.append(own)
    pad = [jnp.zeros((PB, NP), jnp.int32)]
    want = jnp.concatenate(wants + pad, axis=0)
    own = jnp.concatenate(owns + pad, axis=0)
    found = jnp.zeros((8, NP), jnp.int32)
    for w in range(WIN):
        there = pltpu.roll(own, (HP - w) % NP, 1) if w != HP else own
        there = there << w
        for kr in range(PB):
            used = -((want >> (PB * w + kr)) & 1)
            found = found | (used & there[kr : kr + 1, :])
    counts = bits_set(found)
    before = jnp.sum(jnp.where(panel < p0, counts, 0).astype(jnp.float32)).astype(jnp.int32)
    here = jnp.where(panel == p0, 1, 0)
    mask = jnp.sum((found * here).astype(jnp.float32), axis=1, keepdims=True)
    count = jnp.sum((counts * here).astype(jnp.float32), axis=1, keepdims=True).astype(jnp.int32)
    mask = mask.astype(jnp.int32)
    lane = lax.broadcasted_iota(jnp.int32, (8, BS), 1)
    held = jnp.where(lane < 16, (jnp.broadcast_to(mask, (8, BS)) >> (lane & 15)) & 1, 0)
    turn = (2 * HP - p0) & (NP - 1)
    turn = jnp.where(turn > 14, 0, turn)
    col_of = lax.broadcasted_iota(jnp.int32, (BS, BS), 1)
    row_of = lax.broadcasted_iota(jnp.int32, (BS, BS), 0)
    ahead = ((row_of - turn) & 15) < ((col_of - turn) & 15)
    ahead = jnp.where(ahead, 1.0, 0.0).astype(jnp.bfloat16)
    rank = jnp.dot(held.astype(jnp.bfloat16), ahead, preferred_element_type=jnp.float32)
    rank = rank.astype(jnp.int32)
    slot = lax.broadcasted_iota(jnp.int32, (40, BS), 0)
    panels = ((p0 - 2 * HP + lane) & (NP - 1)).astype(jnp.bfloat16)
    slots = lax.broadcasted_iota(jnp.int32, (1, 40), 1)
    start = before
    for r in range(PB):
        taken = (rank[r : r + 1, :] == slot) & (held[r : r + 1, :] > 0)
        taken = jnp.where(taken, 1.0, 0.0).astype(jnp.bfloat16)
        col = lax.dot_general(
            panels, taken, (((1,), (1,)), ((), ())), preferred_element_type=jnp.float32
        )
        cols = jnp.where(slots < count[r : r + 1, :], PB * col[:1].astype(jnp.int32) + c, -1)
        cols_ref[r : r + 1, :] = cols[:, :WIDTH]
        starts_ref[:, r : r + 1] = jnp.broadcast_to(start, (1, 1))
        start = start + count[r : r + 1, :]
    window = lax.broadcasted_iota(jnp.int32, (2 * WIN, NP), 0)
    panels = lax.broadcasted_iota(jnp.int32, (2 * WIN, NP), 1)
    pick = jnp.where(panels == ((p0 - HP + window) & (NP - 1)), 1.0, 0.0).astype(jnp.bfloat16)
    near = lax.dot_general(
        pick,
        turned.astype(jnp.float32).astype(jnp.bfloat16),
        (((1,), (1,)), ((), ())),
        preferred_element_type=jnp.float32,
    )
    map_ref[:WIN, : GROUPS * ROOM] = near[:WIN].astype(jnp.int32)
    map_ref[WIN:, :] = rank


def square_kernel(map_ref, up_ref, over_ref, down_ref, pair_ref, next_ref, swap_ref, far_ref, last_ref, *refs):
    out_ref = refs[0]
    rights = refs[1]
    sums = refs[2 : 2 + PB]
    staged, blank, in_sem, zero_sem, out_sem = refs[2 + PB :]
    p0, c = place()
    core = p0 & 1
    blank[...] = jnp.zeros(blank.shape, blank.dtype)
    for r in range(PB):
        pltpu.make_async_copy(blank, out_ref.at[r, USED:], zero_sem.at[r]).start()
    moves = (
        (pair_ref, 0, HP, HP),
        (pair_ref, 1, 5, 3),
        (next_ref, 0, 2, 6),
        (next_ref, 1, 3, 5),
        (swap_ref, 0, 7, 1),
        (swap_ref, 1, 6, 2),
        (far_ref, 1, 1, 7),
    )
    copies = []
    for n, (ref, half, even, odd) in enumerate(moves):
        w = jnp.where(core == 0, even, odd)
        copies.append(pltpu.make_async_copy(ref.at[half], rights.at[w], in_sem.at[n]))
    for copy in copies:
        copy.start()
    low = pltpu.make_async_copy(far_ref.at[0], rights.at[0], in_sem.at[WIN - 1])
    crossed = pltpu.make_async_copy(last_ref, rights.at[0], in_sem.at[WIN - 1])
    pl.when(core == 0)(low.start)
    pl.when(core == 1)(crossed.start)
    for r in range(PB):
        sums[r][...] = jnp.zeros((USED, BS, BS), jnp.float32)
    for copy in copies:
        copy.wait()
    low.wait()

    def block_step(s0, carry):
        for d in range(GROUPS):
            g = (c + d) & (GROUPS - 1)
            left_ref = (None, up_ref, over_ref, down_ref)[d]
            for r in range(PB):
                w = map_ref[HP, ROOM * g + KG * r + s0]
                slots = []
                for s in range(KG):
                    slots.append(map_ref[WIN + r, map_ref[w, ROOM * c + KG * g + s] + w])
                right = jnp.concatenate([rights[w, g, s] for s in range(KG)], axis=1)
                left = left_ref[r, s0] if d else pair_ref[0, r, s0]
                product = jnp.dot(left, right, preferred_element_type=jnp.float32)
                new = [
                    sums[r][slots[s]] + product[:, BS * s : BS * (s + 1)] for s in range(KG)
                ]
                for s in range(KG):
                    sums[r][slots[s]] = new[s]
        return carry

    lax.fori_loop(0, KG, block_step, 0)
    for r in range(PB):
        staged[r] = sums[r][...].astype(jnp.bfloat16)
        pltpu.make_async_copy(staged.at[r], out_ref.at[r, :USED], out_sem.at[r]).start()
    for r in range(PB):
        pltpu.make_async_copy(blank, out_ref.at[r, USED:], zero_sem.at[r]).wait()
        pltpu.make_async_copy(staged.at[r], out_ref.at[r, :USED], out_sem.at[r]).wait()


VMEM = pl.BlockSpec(memory_space=pltpu.VMEM)
SMEM = pl.BlockSpec(memory_space=pltpu.SMEM)
HBM = pl.BlockSpec(memory_space=pl.ANY)


def near_core(array):
    return pltpu.with_memory_space_constraint(array, pltpu.VMEM)


def spread(cols):
    return pl.pallas_call(
        spread_kernel,
        out_shape=jax.ShapeDtypeStruct((NP, 1, BS), jnp.int32),
        in_specs=[SMEM],
        out_specs=VMEM,
        compiler_params=pltpu.CompilerParams(vmem_limit_bytes=8 << 20),
        name="spread",
    )(cols)


def turned_table(parts):
    return pl.pallas_call(
        turn_kernel,
        out_shape=jax.ShapeDtypeStruct((GROUPS, ROOM, BS), jnp.int32),
        in_specs=[VMEM],
        out_specs=VMEM,
        scratch_shapes=[pltpu.VMEM((NP, BS), jnp.int32)],
        compiler_params=pltpu.CompilerParams(vmem_limit_bytes=8 << 20),
        name="turned_table",
    )(parts)


def indices(table):
    return pl.pallas_call(
        index_kernel,
        out_shape=(
            jax.ShapeDtypeStruct((PB, WIDTH), jnp.int32),
            jax.ShapeDtypeStruct((1, PB), jnp.int32),
            jax.ShapeDtypeStruct((16, BS), jnp.int32),
        ),
        in_specs=[VMEM],
        out_specs=(VMEM, VMEM, VMEM),
        scratch_shapes=[pltpu.VMEM((GROUPS * ROOM, NP), jnp.int32)],
        compiler_params=pltpu.CompilerParams(vmem_limit_bytes=8 << 20),
        name="indices",
    )(table)


def square(where, lefts, pieces):
    return pl.pallas_call(
        square_kernel,
        out_shape=jax.ShapeDtypeStruct((PB, WIDTH, BS, BS), jnp.bfloat16),
        in_specs=[SMEM] + [VMEM] * (len(lefts) + len(pieces)),
        out_specs=HBM,
        scratch_shapes=[
            pltpu.VMEM((WIN, PB, KG, BS, BS), jnp.bfloat16),
        ]
        + [pltpu.VMEM((USED, BS, BS), jnp.float32) for _ in range(PB)]
        + [
            pltpu.VMEM((PB, USED, BS, BS), jnp.bfloat16),
            pltpu.VMEM((WIDTH - USED, BS, BS), jnp.bfloat16),
            pltpu.SemaphoreType.DMA((WIN,)),
            pltpu.SemaphoreType.DMA((PB,)),
            pltpu.SemaphoreType.DMA((PB,)),
        ],
        compiler_params=pltpu.CompilerParams(vmem_limit_bytes=24 << 20),
        name="square",
    )(where, *[near_core(piece) for piece in (*lefts, *pieces)])


def exchange(array, axes):
    return lax.all_to_all(array, axes, 0, 0, tiled=True)


def swapped(block):
    return lax.ppermute(block, "rows_2", [(0, 1), (1, 0)])


def turned(block, distance):
    return lax.ppermute(block, "cols", [((c + distance) % GROUPS, c) for c in range(GROUPS)])


def outward(pair):
    chips = NP // 2
    route = []
    for q in range(chips):
        route.append((2 * q, 2 * ((q + 1) % chips)))
        route.append((2 * q + 1, 2 * ((q - 1) % chips) + 1))
    return lax.ppermute(pair, ROWS, route)


def on_device(blocks, block_cols):
    own = blocks[:, 0]
    parts = exchange(spread(block_cols[:, 0]), ROWS)
    table = exchange(turned_table(parts), "cols")
    columns, starts, where = indices(table)
    partner = swapped(own)
    pair = jnp.stack([own, partner])
    near = outward(pair)
    up = turned(own, 1)
    down = turned(own, 3)
    over = turned(own, 2)
    far = outward(near)
    swap = swapped(near)
    last = lax.ppermute(far[1], "rows_2", [(0, 1)])
    out = square(where, (up, over, down), (pair, near, swap, far, last))
    return out[:, None], columns[:, None], starts.reshape(PB, 1)


def solution(mesh):
    split = Mesh(
        mesh.devices.reshape(16, 4, 2, mesh.shape["cols"]), ("rows_0", "rows_1", "rows_2", "cols")
    )
    return jax.shard_map(
        on_device,
        mesh=split,
        in_specs=(P(ROWS, "cols", None, None, None), P(ROWS, "cols", None)),
        out_specs=(P(ROWS, "cols", None, None, None), P(ROWS, "cols", None), P(ROWS, "cols")),
        check_vma=False,
    )
```

```python
import jax
import jax.numpy as jnp
from jax import lax
from jax.experimental import pallas as pl
from jax.experimental.pallas import tpu as pltpu
from jax.sharding import Mesh
from jax.sharding import PartitionSpec as P

HP = 4
PB = 4
KG = 3
GROUPS = 4
BS = 128
NP = 128
WIDTH = 36
USED = 15
WIN = 2 * HP
ROWS = ("rows_0", "rows_1", "rows_2")
ROOM = 16
FAR = 32
NEAR = 16
FAR_AXES = ("rows_0", "rows_2")
NEAR_AXES = ("rows_1", "cols")


def place():
    return lax.axis_index(ROWS), lax.axis_index("cols")


def spread_kernel(cols_ref, out_ref):
    lane = lax.broadcasted_iota(jnp.int32, (1, BS), 1)
    row = jnp.zeros((1, BS), jnp.int32)
    for r in range(PB):
        for s in range(KG):
            row = jnp.where(lane == KG * r + s, cols_ref[r, s] >> 2, row)
    out_ref[...] = jnp.broadcast_to(row[None], out_ref.shape)


def turn_kernel(in_ref, out_ref, table_ref):
    p0, _ = place()
    table_ref[...] = jnp.zeros((NP, BS), jnp.int32)
    for n in range(FAR):
        spot = 8 * (n // 2) + (p0 & 6) + n % 2
        table_ref[pl.ds(spot, 1), :] = in_ref[n]
    turned = jnp.transpose(table_ref[...])
    out_ref[...] = jnp.broadcast_to(turned[None, :ROOM], out_ref.shape)


def bits_set(x):
    x = x - ((x >> 1) & 0x5555)
    x = (x & 0x3333) + ((x >> 2) & 0x3333)
    x = (x + (x >> 4)) & 0x0F0F
    return (x + (x >> 8)) & 0x1F


def index_kernel(tab_ref, cols_ref, starts_ref, map_ref, turned_ref):
    p0, c = place()
    spot = lax.broadcasted_iota(jnp.int32, (GROUPS * ROOM, NP), 1)
    parts = [tab_ref[GROUPS * n : GROUPS * (n + 1)] for n in range(NEAR // GROUPS)]
    turned = ((parts[0] + parts[1]) + (parts[2] + parts[3])).reshape(GROUPS * ROOM, NP)
    turned = (turned - spot + HP) & (NP - 1)
    turned_ref[...] = turned
    panel = lax.broadcasted_iota(jnp.int32, (1, NP), 1)
    wants = []
    owns = []
    for r in range(PB):
        want = jnp.zeros((1, NP), jnp.int32)
        for g in range(GROUPS):
            for s in range(KG):
                at = ROOM * g + KG * r + s
                want = want | jnp.left_shift(1, PB * turned_ref[at : at + 1, :] + g)
        wants.append(want)
        own = jnp.zeros((1, NP), jnp.int32)
        for s in range(KG):
            own = own | jnp.left_shift(1, turned_ref[pl.ds(ROOM * c + KG * r + s, 1), :])
        owns.append(own)
    pad = [jnp.zeros((PB, NP), jnp.int32)]
    want = jnp.concatenate(wants + pad, axis=0)
    own = jnp.concatenate(owns + pad, axis=0)
    found = jnp.zeros((8, NP), jnp.int32)
    for w in range(WIN):
        there = pltpu.roll(own, (HP - w) % NP, 1) if w != HP else own
        there = there << w
        for kr in range(PB):
            used = -((want >> (PB * w + kr)) & 1)
            found = found | (used & there[kr : kr + 1, :])
    counts = bits_set(found)
    before = jnp.sum(jnp.where(panel < p0, counts, 0).astype(jnp.float32)).astype(jnp.int32)
    here = jnp.where(panel == p0, 1, 0)
    mask = jnp.sum((found * here).astype(jnp.float32), axis=1, keepdims=True)
    count = jnp.sum((counts * here).astype(jnp.float32), axis=1, keepdims=True).astype(jnp.int32)
    mask = mask.astype(jnp.int32)
    lane = lax.broadcasted_iota(jnp.int32, (8, BS), 1)
    held = jnp.where(lane < 16, (jnp.broadcast_to(mask, (8, BS)) >> (lane & 15)) & 1, 0)
    turn = (2 * HP - p0) & (NP - 1)
    turn = jnp.where(turn > 14, 0, turn)
    col_of = lax.broadcasted_iota(jnp.int32, (BS, BS), 1)
    row_of = lax.broadcasted_iota(jnp.int32, (BS, BS), 0)
    ahead = ((row_of - turn) & 15) < ((col_of - turn) & 15)
    ahead = jnp.where(ahead, 1.0, 0.0).astype(jnp.bfloat16)
    rank = jnp.dot(held.astype(jnp.bfloat16), ahead, preferred_element_type=jnp.float32)
    rank = rank.astype(jnp.int32)
    slot = lax.broadcasted_iota(jnp.int32, (40, BS), 0)
    panels = ((p0 - 2 * HP + lane) & (NP - 1)).astype(jnp.bfloat16)
    slots = lax.broadcasted_iota(jnp.int32, (1, 40), 1)
    start = before
    for r in range(PB):
        taken = (rank[r : r + 1, :] == slot) & (held[r : r + 1, :] > 0)
        taken = jnp.where(taken, 1.0, 0.0).astype(jnp.bfloat16)
        col = lax.dot_general(
            panels, taken, (((1,), (1,)), ((), ())), preferred_element_type=jnp.float32
        )
        cols = jnp.where(slots < count[r : r + 1, :], PB * col[:1].astype(jnp.int32) + c, -1)
        cols_ref[r : r + 1, :] = cols[:, :WIDTH]
        starts_ref[:, r : r + 1] = jnp.broadcast_to(start, (1, 1))
        start = start + count[r : r + 1, :]
    window = lax.broadcasted_iota(jnp.int32, (2 * WIN, NP), 0)
    panels = lax.broadcasted_iota(jnp.int32, (2 * WIN, NP), 1)
    pick = jnp.where(panels == ((p0 - HP + window) & (NP - 1)), 1.0, 0.0).astype(jnp.bfloat16)
    near = lax.dot_general(
        pick,
        turned.astype(jnp.float32).astype(jnp.bfloat16),
        (((1,), (1,)), ((), ())),
        preferred_element_type=jnp.float32,
    )
    map_ref[:WIN, : GROUPS * ROOM] = near[:WIN].astype(jnp.int32)
    map_ref[WIN:, :] = rank


def square_kernel(map_ref, up_ref, over_ref, down_ref, pair_ref, next_ref, swap_ref, far_ref, last_ref, *refs):
    out_ref = refs[0]
    rights = refs[1]
    sums = refs[2 : 2 + PB]
    staged, blank, in_sem, zero_sem, out_sem = refs[2 + PB :]
    p0, c = place()
    core = p0 & 1
    blank[...] = jnp.zeros(blank.shape, blank.dtype)
    for r in range(PB):
        pltpu.make_async_copy(blank, out_ref.at[r, USED:], zero_sem.at[r]).start()
    moves = (
        (pair_ref, 0, HP, HP),
        (pair_ref, 1, 5, 3),
        (next_ref, 0, 2, 6),
        (next_ref, 1, 3, 5),
        (swap_ref, 0, 7, 1),
        (swap_ref, 1, 6, 2),
        (far_ref, 1, 1, 7),
    )
    copies = []
    for n, (ref, half, even, odd) in enumerate(moves):
        w = jnp.where(core == 0, even, odd)
        copies.append(pltpu.make_async_copy(ref.at[half], rights.at[w], in_sem.at[n]))
    for copy in copies:
        copy.start()
    low = pltpu.make_async_copy(far_ref.at[0], rights.at[0], in_sem.at[WIN - 1])
    crossed = pltpu.make_async_copy(last_ref, rights.at[0], in_sem.at[WIN - 1])
    pl.when(core == 0)(low.start)
    pl.when(core == 1)(crossed.start)
    for r in range(PB):
        sums[r][...] = jnp.zeros((USED, BS, BS), jnp.float32)
    for copy in copies:
        copy.wait()
    low.wait()

    def block_step(s0, carry):
        for d in range(GROUPS):
            g = (c + d) & (GROUPS - 1)
            left_ref = (None, up_ref, over_ref, down_ref)[d]
            for r in range(PB):
                w = map_ref[HP, ROOM * g + KG * r + s0]
                slots = []
                for s in range(KG):
                    slots.append(map_ref[WIN + r, map_ref[w, ROOM * c + KG * g + s] + w])
                right = jnp.concatenate([rights[w, g, s] for s in range(KG)], axis=1)
                left = left_ref[r, s0] if d else pair_ref[0, r, s0]
                product = jnp.dot(left, right, preferred_element_type=jnp.float32)
                new = [
                    sums[r][slots[s]] + product[:, BS * s : BS * (s + 1)] for s in range(KG)
                ]
                for s in range(KG):
                    sums[r][slots[s]] = new[s]
        return carry

    lax.fori_loop(0, KG, block_step, 0)
    for r in range(PB):
        staged[r] = sums[r][...].astype(jnp.bfloat16)
        pltpu.make_async_copy(staged.at[r], out_ref.at[r, :USED], out_sem.at[r]).start()
    for r in range(PB):
        pltpu.make_async_copy(blank, out_ref.at[r, USED:], zero_sem.at[r]).wait()
        pltpu.make_async_copy(staged.at[r], out_ref.at[r, :USED], out_sem.at[r]).wait()


VMEM = pl.BlockSpec(memory_space=pltpu.VMEM)
SMEM = pl.BlockSpec(memory_space=pltpu.SMEM)
HBM = pl.BlockSpec(memory_space=pl.ANY)


def near_core(array):
    return pltpu.with_memory_space_constraint(array, pltpu.VMEM)


def spread(cols):
    return pl.pallas_call(
        spread_kernel,
        out_shape=jax.ShapeDtypeStruct((FAR, 1, BS), jnp.int32),
        in_specs=[SMEM],
        out_specs=VMEM,
        compiler_params=pltpu.CompilerParams(vmem_limit_bytes=8 << 20),
        name="spread",
    )(cols)


def turned_table(parts):
    return pl.pallas_call(
        turn_kernel,
        out_shape=jax.ShapeDtypeStruct((NEAR, ROOM, BS), jnp.int32),
        in_specs=[VMEM],
        out_specs=VMEM,
        scratch_shapes=[pltpu.VMEM((NP, BS), jnp.int32)],
        compiler_params=pltpu.CompilerParams(vmem_limit_bytes=8 << 20),
        name="turned_table",
    )(parts)


def indices(table):
    return pl.pallas_call(
        index_kernel,
        out_shape=(
            jax.ShapeDtypeStruct((PB, WIDTH), jnp.int32),
            jax.ShapeDtypeStruct((1, PB), jnp.int32),
            jax.ShapeDtypeStruct((16, BS), jnp.int32),
        ),
        in_specs=[VMEM],
        out_specs=(VMEM, VMEM, VMEM),
        scratch_shapes=[pltpu.VMEM((GROUPS * ROOM, NP), jnp.int32)],
        compiler_params=pltpu.CompilerParams(vmem_limit_bytes=8 << 20),
        name="indices",
    )(table)


def square(where, lefts, pieces):
    return pl.pallas_call(
        square_kernel,
        out_shape=jax.ShapeDtypeStruct((PB, WIDTH, BS, BS), jnp.bfloat16),
        in_specs=[SMEM] + [VMEM] * (len(lefts) + len(pieces)),
        out_specs=HBM,
        scratch_shapes=[
            pltpu.VMEM((WIN, PB, KG, BS, BS), jnp.bfloat16),
        ]
        + [pltpu.VMEM((USED, BS, BS), jnp.float32) for _ in range(PB)]
        + [
            pltpu.VMEM((PB, USED, BS, BS), jnp.bfloat16),
            pltpu.VMEM((WIDTH - USED, BS, BS), jnp.bfloat16),
            pltpu.SemaphoreType.DMA((WIN,)),
            pltpu.SemaphoreType.DMA((PB,)),
            pltpu.SemaphoreType.DMA((PB,)),
        ],
        compiler_params=pltpu.CompilerParams(vmem_limit_bytes=24 << 20),
        name="square",
    )(where, *[near_core(piece) for piece in (*lefts, *pieces)])


def exchange(array, axes):
    return lax.all_to_all(array, axes, 0, 0, tiled=True)


def swapped(block):
    return lax.ppermute(block, "rows_2", [(0, 1), (1, 0)])


def turned(block, distance):
    return lax.ppermute(block, "cols", [((c + distance) % GROUPS, c) for c in range(GROUPS)])


def outward(pair):
    chips = NP // 2
    route = []
    for q in range(chips):
        route.append((2 * q, 2 * ((q + 1) % chips)))
        route.append((2 * q + 1, 2 * ((q - 1) % chips) + 1))
    return lax.ppermute(pair, ROWS, route)


def on_device(blocks, block_cols):
    own = blocks[:, 0]
    parts = exchange(spread(block_cols[:, 0]), FAR_AXES)
    table = exchange(turned_table(parts), NEAR_AXES)
    columns, starts, where = indices(table)
    partner = swapped(own)
    pair = jnp.stack([own, partner])
    near = outward(pair)
    up = turned(own, 1)
    down = turned(own, 3)
    over = turned(own, 2)
    far = outward(near)
    swap = swapped(near)
    last = lax.ppermute(far[1], "rows_2", [(0, 1)])
    out = square(where, (up, over, down), (pair, near, swap, far, last))
    return out[:, None], columns[:, None], starts.reshape(PB, 1)


def solution(mesh):
    split = Mesh(
        mesh.devices.reshape(16, 4, 2, mesh.shape["cols"]), ("rows_0", "rows_1", "rows_2", "cols")
    )
    return jax.shard_map(
        on_device,
        mesh=split,
        in_specs=(P(ROWS, "cols", None, None, None), P(ROWS, "cols", None)),
        out_specs=(P(ROWS, "cols", None, None, None), P(ROWS, "cols", None), P(ROWS, "cols")),
        check_vma=False,
    )
```

```python
import jax
import jax.numpy as jnp
from jax import lax
from jax.experimental import pallas as pl
from jax.experimental.pallas import tpu as pltpu
from jax.sharding import Mesh
from jax.sharding import PartitionSpec as P

HP = 4
PB = 4
KG = 3
GROUPS = 4
BS = 128
NP = 128
WIDTH = 36
USED = 15
WIN = 2 * HP
ROWS = ("rows_0", "rows_1", "rows_2")
ROOM = 16
FLOOR = 512
ALL_AXES = (*ROWS, "cols")


def place():
    return lax.axis_index(ROWS), lax.axis_index("cols")


def spread_kernel(cols_ref, out_ref):
    lane = lax.broadcasted_iota(jnp.int32, (1, FLOOR), 1)
    row = jnp.zeros((1, FLOOR), jnp.int32)
    for r in range(PB):
        for s in range(KG):
            row = jnp.where(lane == KG * r + s, cols_ref[r, s] >> 2, row)
    out_ref[0] = row


def bits_set(x):
    x = x - ((x >> 1) & 0x5555)
    x = (x & 0x3333) + ((x >> 2) & 0x3333)
    x = (x + (x >> 4)) & 0x0F0F
    return (x + (x >> 8)) & 0x1F


def index_kernel(tab_ref, cols_ref, starts_ref, map_ref, table_ref, turned_ref):
    p0, c = place()
    spot = lax.broadcasted_iota(jnp.int32, (GROUPS * ROOM, NP), 1)
    for n in range(GROUPS * NP):
        table_ref[n : n + 1, :] = tab_ref[n, :, :BS]
    parts = []
    for g in range(GROUPS):
        parts.append(jnp.transpose(table_ref[pl.ds(g, NP, stride=GROUPS), :])[:ROOM])
    turned = jnp.concatenate(parts, axis=0)
    turned = (turned - spot + HP) & (NP - 1)
    turned_ref[...] = turned
    panel = lax.broadcasted_iota(jnp.int32, (1, NP), 1)
    wants = []
    owns = []
    for r in range(PB):
        want = jnp.zeros((1, NP), jnp.int32)
        for g in range(GROUPS):
            for s in range(KG):
                at = ROOM * g + KG * r + s
                want = want | jnp.left_shift(1, PB * turned_ref[at : at + 1, :] + g)
        wants.append(want)
        own = jnp.zeros((1, NP), jnp.int32)
        for s in range(KG):
            own = own | jnp.left_shift(1, turned_ref[pl.ds(ROOM * c + KG * r + s, 1), :])
        owns.append(own)
    pad = [jnp.zeros((PB, NP), jnp.int32)]
    want = jnp.concatenate(wants + pad, axis=0)
    own = jnp.concatenate(owns + pad, axis=0)
    found = jnp.zeros((8, NP), jnp.int32)
    for w in range(WIN):
        there = pltpu.roll(own, (HP - w) % NP, 1) if w != HP else own
        there = there << w
        for kr in range(PB):
            used = -((want >> (PB * w + kr)) & 1)
            found = found | (used & there[kr : kr + 1, :])
    counts = bits_set(found)
    before = jnp.sum(jnp.where(panel < p0, counts, 0).astype(jnp.float32)).astype(jnp.int32)
    here = jnp.where(panel == p0, 1, 0)
    mask = jnp.sum((found * here).astype(jnp.float32), axis=1, keepdims=True)
    count = jnp.sum((counts * here).astype(jnp.float32), axis=1, keepdims=True).astype(jnp.int32)
    mask = mask.astype(jnp.int32)
    lane = lax.broadcasted_iota(jnp.int32, (8, BS), 1)
    held = jnp.where(lane < 16, (jnp.broadcast_to(mask, (8, BS)) >> (lane & 15)) & 1, 0)
    turn = (2 * HP - p0) & (NP - 1)
    turn = jnp.where(turn > 14, 0, turn)
    col_of = lax.broadcasted_iota(jnp.int32, (BS, BS), 1)
    row_of = lax.broadcasted_iota(jnp.int32, (BS, BS), 0)
    ahead = ((row_of - turn) & 15) < ((col_of - turn) & 15)
    ahead = jnp.where(ahead, 1.0, 0.0).astype(jnp.bfloat16)
    rank = jnp.dot(held.astype(jnp.bfloat16), ahead, preferred_element_type=jnp.float32)
    rank = rank.astype(jnp.int32)
    slot = lax.broadcasted_iota(jnp.int32, (40, BS), 0)
    panels = ((p0 - 2 * HP + lane) & (NP - 1)).astype(jnp.bfloat16)
    slots = lax.broadcasted_iota(jnp.int32, (1, 40), 1)
    start = before
    for r in range(PB):
        taken = (rank[r : r + 1, :] == slot) & (held[r : r + 1, :] > 0)
        taken = jnp.where(taken, 1.0, 0.0).astype(jnp.bfloat16)
        col = lax.dot_general(
            panels, taken, (((1,), (1,)), ((), ())), preferred_element_type=jnp.float32
        )
        cols = jnp.where(slots < count[r : r + 1, :], PB * col[:1].astype(jnp.int32) + c, -1)
        cols_ref[r : r + 1, :] = cols[:, :WIDTH]
        starts_ref[:, r : r + 1] = jnp.broadcast_to(start, (1, 1))
        start = start + count[r : r + 1, :]
    window = lax.broadcasted_iota(jnp.int32, (2 * WIN, NP), 0)
    panels = lax.broadcasted_iota(jnp.int32, (2 * WIN, NP), 1)
    pick = jnp.where(panels == ((p0 - HP + window) & (NP - 1)), 1.0, 0.0).astype(jnp.bfloat16)
    near = lax.dot_general(
        pick,
        turned.astype(jnp.float32).astype(jnp.bfloat16),
        (((1,), (1,)), ((), ())),
        preferred_element_type=jnp.float32,
    )
    map_ref[:WIN, : GROUPS * ROOM] = near[:WIN].astype(jnp.int32)
    map_ref[WIN:, :] = rank


def square_kernel(map_ref, up_ref, over_ref, down_ref, pair_ref, next_ref, swap_ref, far_ref, last_ref, *refs):
    out_ref = refs[0]
    rights = refs[1]
    sums = refs[2 : 2 + PB]
    staged, blank, in_sem, zero_sem, out_sem = refs[2 + PB :]
    p0, c = place()
    core = p0 & 1
    blank[...] = jnp.zeros(blank.shape, blank.dtype)
    for r in range(PB):
        pltpu.make_async_copy(blank, out_ref.at[r, USED:], zero_sem.at[r]).start()
    moves = (
        (pair_ref, 0, HP, HP),
        (pair_ref, 1, 5, 3),
        (next_ref, 0, 2, 6),
        (next_ref, 1, 3, 5),
        (swap_ref, 0, 7, 1),
        (swap_ref, 1, 6, 2),
        (far_ref, 1, 1, 7),
    )
    copies = []
    for n, (ref, half, even, odd) in enumerate(moves):
        w = jnp.where(core == 0, even, odd)
        copies.append(pltpu.make_async_copy(ref.at[half], rights.at[w], in_sem.at[n]))
    for copy in copies:
        copy.start()
    low = pltpu.make_async_copy(far_ref.at[0], rights.at[0], in_sem.at[WIN - 1])
    crossed = pltpu.make_async_copy(last_ref, rights.at[0], in_sem.at[WIN - 1])
    pl.when(core == 0)(low.start)
    pl.when(core == 1)(crossed.start)
    for r in range(PB):
        sums[r][...] = jnp.zeros((USED, BS, BS), jnp.float32)
    for copy in copies:
        copy.wait()
    low.wait()

    def block_step(s0, carry):
        for d in range(GROUPS):
            g = (c + d) & (GROUPS - 1)
            left_ref = (None, up_ref, over_ref, down_ref)[d]
            for r in range(PB):
                w = map_ref[HP, ROOM * g + KG * r + s0]
                slots = []
                for s in range(KG):
                    slots.append(map_ref[WIN + r, map_ref[w, ROOM * c + KG * g + s] + w])
                right = jnp.concatenate([rights[w, g, s] for s in range(KG)], axis=1)
                left = left_ref[r, s0] if d else pair_ref[0, r, s0]
                product = jnp.dot(left, right, preferred_element_type=jnp.float32)
                new = [
                    sums[r][slots[s]] + product[:, BS * s : BS * (s + 1)] for s in range(KG)
                ]
                for s in range(KG):
                    sums[r][slots[s]] = new[s]
        return carry

    lax.fori_loop(0, KG, block_step, 0)
    for r in range(PB):
        staged[r] = sums[r][...].astype(jnp.bfloat16)
        pltpu.make_async_copy(staged.at[r], out_ref.at[r, :USED], out_sem.at[r]).start()
    for r in range(PB):
        pltpu.make_async_copy(blank, out_ref.at[r, USED:], zero_sem.at[r]).wait()
        pltpu.make_async_copy(staged.at[r], out_ref.at[r, :USED], out_sem.at[r]).wait()


VMEM = pl.BlockSpec(memory_space=pltpu.VMEM)
SMEM = pl.BlockSpec(memory_space=pltpu.SMEM)
HBM = pl.BlockSpec(memory_space=pl.ANY)


def near_core(array):
    return pltpu.with_memory_space_constraint(array, pltpu.VMEM)


def spread(cols):
    return pl.pallas_call(
        spread_kernel,
        out_shape=jax.ShapeDtypeStruct((1, 1, FLOOR), jnp.int32),
        in_specs=[SMEM],
        out_specs=VMEM,
        compiler_params=pltpu.CompilerParams(vmem_limit_bytes=8 << 20),
        name="spread",
    )(cols)


def indices(table):
    return pl.pallas_call(
        index_kernel,
        out_shape=(
            jax.ShapeDtypeStruct((PB, WIDTH), jnp.int32),
            jax.ShapeDtypeStruct((1, PB), jnp.int32),
            jax.ShapeDtypeStruct((16, BS), jnp.int32),
        ),
        in_specs=[VMEM],
        out_specs=(VMEM, VMEM, VMEM),
        scratch_shapes=[
            pltpu.VMEM((GROUPS * NP, BS), jnp.int32),
            pltpu.VMEM((GROUPS * ROOM, NP), jnp.int32),
        ],
        compiler_params=pltpu.CompilerParams(vmem_limit_bytes=8 << 20),
        name="indices",
    )(table)


def square(where, lefts, pieces):
    return pl.pallas_call(
        square_kernel,
        out_shape=jax.ShapeDtypeStruct((PB, WIDTH, BS, BS), jnp.bfloat16),
        in_specs=[SMEM] + [VMEM] * (len(lefts) + len(pieces)),
        out_specs=HBM,
        scratch_shapes=[
            pltpu.VMEM((WIN, PB, KG, BS, BS), jnp.bfloat16),
        ]
        + [pltpu.VMEM((USED, BS, BS), jnp.float32) for _ in range(PB)]
        + [
            pltpu.VMEM((PB, USED, BS, BS), jnp.bfloat16),
            pltpu.VMEM((WIDTH - USED, BS, BS), jnp.bfloat16),
            pltpu.SemaphoreType.DMA((WIN,)),
            pltpu.SemaphoreType.DMA((PB,)),
            pltpu.SemaphoreType.DMA((PB,)),
        ],
        compiler_params=pltpu.CompilerParams(vmem_limit_bytes=24 << 20),
        name="square",
    )(where, *[near_core(piece) for piece in (*lefts, *pieces)])


def swapped(block):
    return lax.ppermute(block, "rows_2", [(0, 1), (1, 0)])


def turned(block, distance):
    return lax.ppermute(block, "cols", [((c + distance) % GROUPS, c) for c in range(GROUPS)])


def outward(pair):
    chips = NP // 2
    route = []
    for q in range(chips):
        route.append((2 * q, 2 * ((q + 1) % chips)))
        route.append((2 * q + 1, 2 * ((q - 1) % chips) + 1))
    return lax.ppermute(pair, ROWS, route)


def on_device(blocks, block_cols):
    own = blocks[:, 0]
    table = lax.all_gather(spread(block_cols[:, 0]), ALL_AXES, axis=0, tiled=True)
    columns, starts, where = indices(table)
    partner = swapped(own)
    pair = jnp.stack([own, partner])
    near = outward(pair)
    up = turned(own, 1)
    down = turned(own, 3)
    over = turned(own, 2)
    far = outward(near)
    swap = swapped(near)
    last = lax.ppermute(far[1], "rows_2", [(0, 1)])
    out = square(where, (up, over, down), (pair, near, swap, far, last))
    return out[:, None], columns[:, None], starts.reshape(PB, 1)


def solution(mesh):
    split = Mesh(
        mesh.devices.reshape(16, 4, 2, mesh.shape["cols"]), ("rows_0", "rows_1", "rows_2", "cols")
    )
    return jax.shard_map(
        on_device,
        mesh=split,
        in_specs=(P(ROWS, "cols", None, None, None), P(ROWS, "cols", None)),
        out_specs=(P(ROWS, "cols", None, None, None), P(ROWS, "cols", None), P(ROWS, "cols")),
        check_vma=False,
    )
```

```python
import jax
import jax.numpy as jnp
from jax import lax
from jax.experimental import pallas as pl
from jax.experimental.pallas import tpu as pltpu
from jax.sharding import Mesh
from jax.sharding import PartitionSpec as P

HP = 4
PB = 4
KG = 3
GROUPS = 4
BS = 128
NP = 128
WIDTH = 36
USED = 15
WIN = 2 * HP
ROWS = ("rows_0", "rows_1", "rows_2")
ROOM = 16
FAR = 32
NEAR = 16
FAR_AXES = ("rows_0", "rows_2")
NEAR_AXES = ("rows_1", "cols")


def place():
    return lax.axis_index(ROWS), lax.axis_index("cols")


def spread_kernel(cols_ref, out_ref):
    lane = lax.broadcasted_iota(jnp.int32, (1, BS), 1)
    row = jnp.zeros((1, BS), jnp.int32)
    for r in range(PB):
        for s in range(KG):
            row = jnp.where(lane == KG * r + s, cols_ref[s, 0, r] >> 2, row)
    out_ref[...] = jnp.broadcast_to(row[None], out_ref.shape)


def turn_kernel(in_ref, out_ref, table_ref):
    p0, _ = place()
    table_ref[...] = jnp.zeros((NP, BS), jnp.int32)
    for n in range(FAR):
        spot = 8 * (n // 2) + (p0 & 6) + n % 2
        table_ref[pl.ds(spot, 1), :] = in_ref[n]
    turned = jnp.transpose(table_ref[...])
    out_ref[...] = jnp.broadcast_to(turned[None, :ROOM], out_ref.shape)


def bits_set(x):
    x = x - ((x >> 1) & 0x5555)
    x = (x & 0x3333) + ((x >> 2) & 0x3333)
    x = (x + (x >> 4)) & 0x0F0F
    return (x + (x >> 8)) & 0x1F


def index_kernel(tab_ref, cols_ref, starts_ref, map_ref, turned_ref):
    p0, c = place()
    spot = lax.broadcasted_iota(jnp.int32, (GROUPS * ROOM, NP), 1)
    parts = [tab_ref[GROUPS * n : GROUPS * (n + 1)] for n in range(NEAR // GROUPS)]
    turned = ((parts[0] + parts[1]) + (parts[2] + parts[3])).reshape(GROUPS * ROOM, NP)
    turned = (turned - spot + HP) & (NP - 1)
    turned_ref[...] = turned
    panel = lax.broadcasted_iota(jnp.int32, (1, NP), 1)
    wants = []
    owns = []
    for r in range(PB):
        want = jnp.zeros((1, NP), jnp.int32)
        for g in range(GROUPS):
            for s in range(KG):
                at = ROOM * g + KG * r + s
                want = want | jnp.left_shift(1, PB * turned_ref[at : at + 1, :] + g)
        wants.append(want)
        own = jnp.zeros((1, NP), jnp.int32)
        for s in range(KG):
            own = own | jnp.left_shift(1, turned_ref[pl.ds(ROOM * c + KG * r + s, 1), :])
        owns.append(own)
    pad = [jnp.zeros((PB, NP), jnp.int32)]
    want = jnp.concatenate(wants + pad, axis=0)
    own = jnp.concatenate(owns + pad, axis=0)
    found = jnp.zeros((8, NP), jnp.int32)
    for w in range(WIN):
        there = pltpu.roll(own, (HP - w) % NP, 1) if w != HP else own
        there = there << w
        for kr in range(PB):
            used = -((want >> (PB * w + kr)) & 1)
            found = found | (used & there[kr : kr + 1, :])
    counts = bits_set(found)
    before = jnp.sum(jnp.where(panel < p0, counts, 0).astype(jnp.float32)).astype(jnp.int32)
    here = jnp.where(panel == p0, 1, 0)
    mask = jnp.sum((found * here).astype(jnp.float32), axis=1, keepdims=True)
    count = jnp.sum((counts * here).astype(jnp.float32), axis=1, keepdims=True).astype(jnp.int32)
    mask = mask.astype(jnp.int32)
    lane = lax.broadcasted_iota(jnp.int32, (8, BS), 1)
    held = jnp.where(lane < 16, (jnp.broadcast_to(mask, (8, BS)) >> (lane & 15)) & 1, 0)
    turn = (2 * HP - p0) & (NP - 1)
    turn = jnp.where(turn > 14, 0, turn)
    col_of = lax.broadcasted_iota(jnp.int32, (BS, BS), 1)
    row_of = lax.broadcasted_iota(jnp.int32, (BS, BS), 0)
    ahead = ((row_of - turn) & 15) < ((col_of - turn) & 15)
    ahead = jnp.where(ahead, 1.0, 0.0).astype(jnp.bfloat16)
    rank = jnp.dot(held.astype(jnp.bfloat16), ahead, preferred_element_type=jnp.float32)
    rank = rank.astype(jnp.int32)
    slot = lax.broadcasted_iota(jnp.int32, (40, BS), 0)
    panels = ((p0 - 2 * HP + lane) & (NP - 1)).astype(jnp.bfloat16)
    slots = lax.broadcasted_iota(jnp.int32, (1, 40), 1)
    start = before
    for r in range(PB):
        taken = (rank[r : r + 1, :] == slot) & (held[r : r + 1, :] > 0)
        taken = jnp.where(taken, 1.0, 0.0).astype(jnp.bfloat16)
        col = lax.dot_general(
            panels, taken, (((1,), (1,)), ((), ())), preferred_element_type=jnp.float32
        )
        cols = jnp.where(slots < count[r : r + 1, :], PB * col[:1].astype(jnp.int32) + c, -1)
        cols_ref[r : r + 1, :] = cols[:, :WIDTH]
        starts_ref[:, r : r + 1] = jnp.broadcast_to(start, (1, 1))
        start = start + count[r : r + 1, :]
    window = lax.broadcasted_iota(jnp.int32, (2 * WIN, NP), 0)
    panels = lax.broadcasted_iota(jnp.int32, (2 * WIN, NP), 1)
    pick = jnp.where(panels == ((p0 - HP + window) & (NP - 1)), 1.0, 0.0).astype(jnp.bfloat16)
    near = lax.dot_general(
        pick,
        turned.astype(jnp.float32).astype(jnp.bfloat16),
        (((1,), (1,)), ((), ())),
        preferred_element_type=jnp.float32,
    )
    map_ref[:WIN, : GROUPS * ROOM] = near[:WIN].astype(jnp.int32)
    map_ref[WIN:, :] = rank


def square_kernel(
    map_ref, up_ref, over_ref, down_ref, trio_ref, swap_ref, back_ref, far_ref, out_ref, *refs
):
    rights, sums, staged, blank, in_sem, zero_sem, out_sem = refs
    p0, c = place()
    core = p0 & 1
    blank[...] = jnp.zeros(blank.shape, blank.dtype)
    for r in range(PB):
        pltpu.make_async_copy(blank, out_ref.at[r, USED:], zero_sem.at[r]).start()
    moves = (
        (trio_ref.at[0], HP, HP),
        (trio_ref.at[1], 2, 2),
        (trio_ref.at[2], 6, 6),
        (swap_ref.at[0], 5, 3),
        (swap_ref.at[1], 3, 1),
        (swap_ref.at[2], 7, 5),
        (back_ref, 0, 0),
        (far_ref, 1, 7),
    )
    copies = []
    for n, (ref, even, odd) in enumerate(moves):
        w = even if even == odd else jnp.where(core == 0, even, odd)
        copies.append(pltpu.make_async_copy(ref, rights.at[w], in_sem.at[n]))
    for copy in copies:
        copy.start()
    sums[...] = jnp.zeros(sums.shape, jnp.float32)
    for copy in copies:
        copy.wait()

    def row_step(r, carry):
        for d in range(GROUPS):
            g = (c + d) & (GROUPS - 1)
            left_ref = (trio_ref.at[0], up_ref, over_ref, down_ref)[d]
            for s0 in range(KG):
                w = map_ref[HP, ROOM * g + KG * r + s0]
                slots = []
                for s in range(KG):
                    slots.append(map_ref[WIN + r, map_ref[w, ROOM * c + KG * g + s] + w])
                right = jnp.concatenate([rights[w, g, s] for s in range(KG)], axis=1)
                product = jnp.dot(left_ref[r, s0], right, preferred_element_type=jnp.float32)
                new = [
                    sums[r, slots[s]] + product[:, BS * s : BS * (s + 1)] for s in range(KG)
                ]
                for s in range(KG):
                    sums[r, slots[s]] = new[s]
        staged[r] = sums[r].astype(jnp.bfloat16)
        pltpu.make_async_copy(staged.at[r], out_ref.at[r, :USED], out_sem.at[r]).start()
        return carry

    lax.fori_loop(0, PB, row_step, 0)
    for r in range(PB):
        pltpu.make_async_copy(blank, out_ref.at[r, USED:], zero_sem.at[r]).wait()
        pltpu.make_async_copy(staged.at[r], out_ref.at[r, :USED], out_sem.at[r]).wait()


VMEM = pl.BlockSpec(memory_space=pltpu.VMEM)
SMEM = pl.BlockSpec(memory_space=pltpu.SMEM)
HBM = pl.BlockSpec(memory_space=pl.ANY)


def near_core(array):
    return pltpu.with_memory_space_constraint(array, pltpu.VMEM)


def spread(cols):
    return pl.pallas_call(
        spread_kernel,
        out_shape=jax.ShapeDtypeStruct((FAR, 1, BS), jnp.int32),
        in_specs=[SMEM],
        out_specs=VMEM,
        compiler_params=pltpu.CompilerParams(vmem_limit_bytes=8 << 20),
        name="spread",
    )(cols)


def turned_table(parts):
    return pl.pallas_call(
        turn_kernel,
        out_shape=jax.ShapeDtypeStruct((NEAR, ROOM, BS), jnp.int32),
        in_specs=[VMEM],
        out_specs=VMEM,
        scratch_shapes=[pltpu.VMEM((NP, BS), jnp.int32)],
        compiler_params=pltpu.CompilerParams(vmem_limit_bytes=8 << 20),
        name="turned_table",
    )(parts)


def indices(table):
    return pl.pallas_call(
        index_kernel,
        out_shape=(
            jax.ShapeDtypeStruct((PB, WIDTH), jnp.int32),
            jax.ShapeDtypeStruct((1, PB), jnp.int32),
            jax.ShapeDtypeStruct((16, BS), jnp.int32),
        ),
        in_specs=[VMEM],
        out_specs=(VMEM, VMEM, VMEM),
        scratch_shapes=[pltpu.VMEM((GROUPS * ROOM, NP), jnp.int32)],
        compiler_params=pltpu.CompilerParams(vmem_limit_bytes=8 << 20),
        name="indices",
    )(table)


def square(where, lefts, pieces):
    return pl.pallas_call(
        square_kernel,
        out_shape=jax.ShapeDtypeStruct((PB, WIDTH, BS, BS), jnp.bfloat16),
        in_specs=[SMEM] + [VMEM] * (len(lefts) + len(pieces)),
        out_specs=HBM,
        scratch_shapes=[
            pltpu.VMEM((WIN, PB, KG, BS, BS), jnp.bfloat16),
            pltpu.VMEM((PB, USED, BS, BS), jnp.float32),
            pltpu.VMEM((PB, USED, BS, BS), jnp.bfloat16),
            pltpu.VMEM((WIDTH - USED, BS, BS), jnp.bfloat16),
            pltpu.SemaphoreType.DMA((WIN,)),
            pltpu.SemaphoreType.DMA((PB,)),
            pltpu.SemaphoreType.DMA((PB,)),
        ],
        compiler_params=pltpu.CompilerParams(vmem_limit_bytes=24 << 20),
        name="square",
    )(where, *[near_core(piece) for piece in (*lefts, *pieces)])


def exchange(array, axes):
    return lax.all_to_all(array, axes, 0, 0, tiled=True)


def swapped(block):
    return lax.ppermute(block, "rows_2", [(0, 1), (1, 0)])


def turned(block, distance):
    return lax.ppermute(block, "cols", [((c + distance) % GROUPS, c) for c in range(GROUPS)])


def sent_on(block, chips, crossed=False):
    count = NP // 2
    route = []
    for q in range(count):
        for core in range(2):
            step = chips * (2 * core - 1) if crossed else chips
            route.append((2 * q + core, 2 * ((q + step) % count) + (core ^ crossed)))
    return lax.ppermute(block, ROWS, route)


def on_device(blocks, block_cols):
    own = blocks[:, 0]
    parts = exchange(spread(block_cols.transpose(2, 1, 0)), FAR_AXES)
    table = exchange(turned_table(parts), NEAR_AXES)
    columns, starts, where = indices(table)
    behind = sent_on(own, 1)
    ahead = sent_on(own, -1)
    far = sent_on(own, 2, True)
    over = turned(own, 2)
    up = turned(own, 1)
    down = turned(own, 3)
    back = sent_on(behind, 1)
    trio = jnp.stack([own, behind, ahead])
    swap = swapped(trio)
    out = square(where, (up, over, down), (trio, swap, back, far))
    return out[:, None], columns[:, None], starts.reshape(PB, 1)


def solution(mesh):
    split = Mesh(
        mesh.devices.reshape(16, 4, 2, mesh.shape["cols"]), ("rows_0", "rows_1", "rows_2", "cols")
    )
    return jax.shard_map(
        on_device,
        mesh=split,
        in_specs=(P(ROWS, "cols", None, None, None), P(ROWS, "cols", None)),
        out_specs=(P(ROWS, "cols", None, None, None), P(ROWS, "cols", None), P(ROWS, "cols")),
        check_vma=False,
    )
```

```python
import jax
import jax.numpy as jnp
from jax import lax
from jax.experimental import pallas as pl
from jax.experimental.pallas import tpu as pltpu
from jax.sharding import Mesh
from jax.sharding import PartitionSpec as P

HP = 4
PB = 4
KG = 3
GROUPS = 4
BS = 128
NP = 128
WIDTH = 36
USED = 15
WIN = 2 * HP
ROOM = 16
FULL = PB * KG * BS
LONG = FULL + ROOM
ROWS = ("rows_0", "rows_1", "rows_2")


def place():
    return lax.axis_index(ROWS), lax.axis_index("cols")


def spread_kernel(in_ref, out_ref):
    lane = lax.broadcasted_iota(jnp.int32, (1, BS), 1)
    row = jnp.zeros((1, BS), jnp.float32)
    for g in range(GROUPS):
        part = in_ref[g].astype(jnp.float32)[:1]
        row = row + pltpu.roll(jnp.where(lane < PB * KG, part, 0.0), ROOM * g, 1)
    out_ref[...] = jnp.broadcast_to(row.astype(jnp.int32)[None], out_ref.shape)


def bits_set(x):
    x = x - ((x >> 1) & 0x5555)
    x = (x & 0x3333) + ((x >> 2) & 0x3333)
    x = (x + (x >> 4)) & 0x0F0F
    return (x + (x >> 8)) & 0x1F


def starts_kernel(tab_ref, starts_ref, table_ref, turned_ref):
    p0, c = place()
    for n in range(NP):
        table_ref[n : n + 1, :] = tab_ref[n]
    panel = lax.broadcasted_iota(jnp.int32, (1, NP), 1)
    turned_ref[...] = (jnp.transpose(table_ref[...]) - panel + HP) & (NP - 1)
    wants = []
    owns = []
    for r in range(PB):
        want = jnp.zeros((1, NP), jnp.int32)
        for g in range(GROUPS):
            for s in range(KG):
                at = ROOM * g + KG * r + s
                want = want | jnp.left_shift(1, PB * turned_ref[at : at + 1, :] + g)
        wants.append(want)
        own = jnp.zeros((1, NP), jnp.int32)
        for s in range(KG):
            own = own | jnp.left_shift(1, turned_ref[pl.ds(ROOM * c + KG * r + s, 1), :])
        owns.append(own)
    pad = [jnp.zeros((PB, NP), jnp.int32)]
    want = jnp.concatenate(wants + pad, axis=0)
    own = jnp.concatenate(owns + pad, axis=0)
    found = jnp.zeros((8, NP), jnp.int32)
    for w in range(WIN):
        there = pltpu.roll(own, (HP - w) % NP, 1) if w != HP else own
        there = there << w
        for kr in range(PB):
            used = -((want >> (PB * w + kr)) & 1)
            found = found | (used & there[kr : kr + 1, :])
    counts = bits_set(found)
    before = jnp.sum(jnp.where(panel < p0, counts, 0).astype(jnp.float32)).astype(jnp.int32)
    here = jnp.where(panel == p0, 1, 0)
    count = jnp.sum((counts * here).astype(jnp.float32), axis=1, keepdims=True).astype(jnp.int32)
    start = before
    for r in range(PB):
        starts_ref[:, r : r + 1] = jnp.broadcast_to(start, (1, 1))
        start = start + count[r : r + 1, :]


def find_slots(lefts, rights, cols_ref, map_ref):
    p0, c = place()
    side = lax.broadcasted_iota(jnp.int32, (WIN, 1), 0)
    there = [rights[w, FULL:LONG].astype(jnp.float32)[:1] for w in range(WIN)]
    there = jnp.concatenate(there, axis=0).astype(jnp.int32)
    there = (there - (p0 + side) + 2 * HP) & (NP - 1)
    here = [lefts[g, FULL:LONG].astype(jnp.float32)[:1] for g in range(GROUPS)]
    here = jnp.concatenate(here + here, axis=0).astype(jnp.int32)
    here = (here - p0 + HP) & (NP - 1)
    map_ref[:WIN] = there
    map_ref[WIN : WIN + PB] = here[:GROUPS]
    group = lax.broadcasted_iota(jnp.int32, (WIN, 1), 0) & (GROUPS - 1)
    want_bits = jnp.left_shift(1, (PB * here + group) & 31)
    want_bits = want_bits[:1] | want_bits[1:2] | want_bits[2:3] | want_bits[3:4]
    own_bits = jnp.left_shift(1, there & 31)
    rows = []
    for r in range(PB):
        want = jnp.zeros((1, 1), jnp.int32)
        for s in range(KG):
            want = want | want_bits[:, KG * r + s : KG * r + s + 1]
        found = jnp.zeros((WIN, 1), jnp.int32)
        for kr in range(PB):
            own = jnp.zeros((WIN, 1), jnp.int32)
            for s in range(KG):
                own = own | own_bits[:, KG * kr + s : KG * kr + s + 1]
            used = -((want >> (PB * side + kr)) & 1)
            found = found | (used & (own << side))
        found = found[:4] | found[4:]
        found = found[:2] | found[2:]
        rows.append(found[:1] | found[1:])
    mask = jnp.concatenate(rows + rows, axis=0)
    count = bits_set(mask)
    lane = lax.broadcasted_iota(jnp.int32, (8, BS), 1)
    held = jnp.where(lane < 16, (jnp.broadcast_to(mask, (8, BS)) >> (lane & 15)) & 1, 0)
    turn = (2 * HP - p0) & (NP - 1)
    turn = jnp.where(turn > 14, 0, turn)
    col_of = lax.broadcasted_iota(jnp.int32, (BS, BS), 1)
    row_of = lax.broadcasted_iota(jnp.int32, (BS, BS), 0)
    ahead = ((row_of - turn) & 15) < ((col_of - turn) & 15)
    ahead = jnp.where(ahead, 1.0, 0.0).astype(jnp.bfloat16)
    rank = jnp.dot(
        held.astype(jnp.float32).astype(jnp.bfloat16), ahead, preferred_element_type=jnp.float32
    )
    rank = rank.astype(jnp.int32)
    map_ref[WIN + PB :] = rank[:PB]
    slot = lax.broadcasted_iota(jnp.int32, (40, BS), 0)
    panels = ((p0 - 2 * HP + lane) & (NP - 1)).astype(jnp.float32).astype(jnp.bfloat16)
    slots = lax.broadcasted_iota(jnp.int32, (1, 40), 1)
    for r in range(PB):
        taken = (rank[r : r + 1, :] == slot) & (held[r : r + 1, :] > 0)
        taken = jnp.where(taken, 1.0, 0.0).astype(jnp.bfloat16)
        col = lax.dot_general(
            panels, taken, (((1,), (1,)), ((), ())), preferred_element_type=jnp.float32
        )
        cols = jnp.where(slots < count[r : r + 1, :], PB * col[:1].astype(jnp.int32) + c, -1)
        cols_ref[r : r + 1, :] = cols[:, :WIDTH]


def square_kernel(
    lefts, trio_ref, swap_ref, back_ref, far_ref, out_ref, cols_ref, *refs
):
    rights, sums, staged, blank, found, map_ref, map_sem, in_sem, zero_sem, out_sem = refs
    p0, _ = place()
    core = p0 & 1
    blank[...] = jnp.zeros(blank.shape, blank.dtype)
    for r in range(PB):
        pltpu.make_async_copy(blank, out_ref.at[r, USED:], zero_sem.at[r]).start()
    moves = (
        (trio_ref.at[0], HP, HP),
        (trio_ref.at[1], 2, 2),
        (trio_ref.at[2], 6, 6),
        (swap_ref.at[0], 5, 3),
        (swap_ref.at[1], 3, 1),
        (swap_ref.at[2], 7, 5),
        (back_ref, 0, 0),
        (far_ref, 1, 7),
    )
    copies = []
    for n, (ref, even, odd) in enumerate(moves):
        w = even if even == odd else jnp.where(core == 0, even, odd)
        copies.append(pltpu.make_async_copy(ref, rights.at[w], in_sem.at[n]))
    for copy in copies:
        copy.start()
    for copy in copies:
        copy.wait()
    find_slots(lefts, rights, cols_ref, found)
    told = pltpu.make_async_copy(found, map_ref, map_sem)
    told.start()
    sums[...] = jnp.zeros(sums.shape, jnp.float32)
    told.wait()

    def row_step(r, carry):
        for g in range(GROUPS):
            for s0 in range(KG):
                w = map_ref[WIN + g, KG * r + s0]
                slots = []
                right = []
                for s in range(KG):
                    slots.append(map_ref[WIN + PB + r, map_ref[w, KG * g + s] + w])
                    right.append(rights[w, BS * (KG * g + s) : BS * (KG * g + s + 1)])
                right = jnp.concatenate(right, axis=1)
                left = lefts[g, pl.ds(pl.multiple_of(BS * (KG * r + s0), BS), BS)]
                product = jnp.dot(left, right, preferred_element_type=jnp.float32)
                new = [
                    sums[r, slots[s]] + product[:, BS * s : BS * (s + 1)] for s in range(KG)
                ]
                for s in range(KG):
                    sums[r, slots[s]] = new[s]
        staged[r] = sums[r].astype(jnp.bfloat16)
        pltpu.make_async_copy(staged.at[r], out_ref.at[r, :USED], out_sem.at[r]).start()
        return carry

    lax.fori_loop(0, PB, row_step, 0)
    for r in range(PB):
        pltpu.make_async_copy(blank, out_ref.at[r, USED:], zero_sem.at[r]).wait()
        pltpu.make_async_copy(staged.at[r], out_ref.at[r, :USED], out_sem.at[r]).wait()


VMEM = pl.BlockSpec(memory_space=pltpu.VMEM)
SMEM = pl.BlockSpec(memory_space=pltpu.SMEM)
HBM = pl.BlockSpec(memory_space=pl.ANY)


def near_core(array):
    return pltpu.with_memory_space_constraint(array, pltpu.VMEM)


def spread(parts):
    return pl.pallas_call(
        spread_kernel,
        out_shape=jax.ShapeDtypeStruct((NP, 1, BS), jnp.int32),
        in_specs=[VMEM],
        out_specs=VMEM,
        compiler_params=pltpu.CompilerParams(vmem_limit_bytes=8 << 20),
        name="spread",
    )(parts)


def starts_of(table):
    return pl.pallas_call(
        starts_kernel,
        out_shape=jax.ShapeDtypeStruct((1, PB), jnp.int32),
        in_specs=[VMEM],
        out_specs=VMEM,
        scratch_shapes=[pltpu.VMEM((NP, BS), jnp.int32), pltpu.VMEM((BS, NP), jnp.int32)],
        compiler_params=pltpu.CompilerParams(vmem_limit_bytes=8 << 20),
        name="starts",
    )(table)


def square(left, pieces):
    return pl.pallas_call(
        square_kernel,
        out_shape=(
            jax.ShapeDtypeStruct((PB, WIDTH, BS, BS), jnp.bfloat16),
            jax.ShapeDtypeStruct((PB, WIDTH), jnp.int32),
        ),
        in_specs=[VMEM] * (1 + len(pieces)),
        out_specs=(HBM, VMEM),
        scratch_shapes=[
            pltpu.VMEM((WIN, LONG, BS), jnp.bfloat16),
            pltpu.VMEM((PB, USED, BS, BS), jnp.float32),
            pltpu.VMEM((PB, USED, BS, BS), jnp.bfloat16),
            pltpu.VMEM((WIDTH - USED, BS, BS), jnp.bfloat16),
            pltpu.VMEM((2 * WIN, BS), jnp.int32),
            pltpu.SMEM((2 * WIN, BS), jnp.int32),
            pltpu.SemaphoreType.DMA,
            pltpu.SemaphoreType.DMA((WIN,)),
            pltpu.SemaphoreType.DMA((PB,)),
            pltpu.SemaphoreType.DMA((PB,)),
        ],
        compiler_params=pltpu.CompilerParams(vmem_limit_bytes=24 << 20),
        name="square",
    )(near_core(left), *[near_core(piece) for piece in pieces])


def exchange(array, axes):
    return lax.all_to_all(array, axes, 0, 0, tiled=True)


def swapped(block):
    return lax.ppermute(block, "rows_2", [(0, 1), (1, 0)])


def sent_on(block, chips, crossed=False):
    count = NP // 2
    route = []
    for q in range(count):
        for core in range(2):
            step = chips * (2 * core - 1) if crossed else chips
            route.append((2 * q + core, 2 * ((q + step) % count) + (core ^ crossed)))
    return lax.ppermute(block, ROWS, route)


def on_device(blocks, block_cols):
    tail = (block_cols.reshape(1, PB * KG) >> 2).astype(jnp.bfloat16)
    tail = jnp.pad(tail, ((0, ROOM - 1), (0, BS - PB * KG)))
    own = jnp.concatenate([blocks.reshape(FULL, BS), tail], axis=0)
    behind = sent_on(own, 1)
    left = exchange(jnp.broadcast_to(own[None], (GROUPS, LONG, BS)), "cols")
    far = sent_on(own, 2, True)
    ahead = sent_on(own, -1)
    back = sent_on(behind, 1)
    trio = jnp.stack([own, behind, ahead])
    swap = swapped(trio)
    table = exchange(spread(left[:, FULL:]), ROWS)
    starts = starts_of(table)
    out, columns = square(left, (trio, swap, back, far))
    return out[:, None], columns[:, None], starts.reshape(PB, 1)


def solution(mesh):
    split = Mesh(
        mesh.devices.reshape(16, 4, 2, mesh.shape["cols"]), ("rows_0", "rows_1", "rows_2", "cols")
    )
    return jax.shard_map(
        on_device,
        mesh=split,
        in_specs=(P(ROWS, "cols", None, None, None), P(ROWS, "cols", None)),
        out_specs=(P(ROWS, "cols", None, None, None), P(ROWS, "cols", None), P(ROWS, "cols")),
        check_vma=False,
    )
```

```python
import jax
import jax.numpy as jnp
from jax import lax
from jax.experimental import pallas as pl
from jax.experimental.pallas import tpu as pltpu
from jax.sharding import Mesh
from jax.sharding import PartitionSpec as P

HP = 4
PB = 4
KG = 3
GROUPS = 4
BS = 128
NP = 128
WIDTH = 36
USED = 15
WIN = 2 * HP
ROWS = ("rows_0", "rows_1", "rows_2")
ROOM = 16
FAR = 32
NEAR = 16
FAR_AXES = ("rows_0", "rows_2")
NEAR_AXES = ("rows_1", "cols")


def place():
    return lax.axis_index(ROWS), lax.axis_index("cols")


def spread_kernel(held_ref, out_ref, cols_ref, sem):
    copy = pltpu.make_async_copy(held_ref, cols_ref, sem)
    copy.start()
    copy.wait()
    lane = lax.broadcasted_iota(jnp.int32, (1, BS), 1)
    row = jnp.zeros((1, BS), jnp.int32)
    for r in range(PB):
        for s in range(KG):
            row = jnp.where(lane == KG * r + s, cols_ref[s, 0, r] >> 2, row)
    out_ref[...] = jnp.broadcast_to(row[None], out_ref.shape)


def turn_kernel(in_ref, out_ref, table_ref):
    p0, _ = place()
    table_ref[...] = jnp.zeros((NP, BS), jnp.int32)
    for n in range(FAR):
        spot = 8 * (n // 2) + (p0 & 6) + n % 2
        table_ref[pl.ds(spot, 1), :] = in_ref[n]
    turned = jnp.transpose(table_ref[...])
    out_ref[...] = jnp.broadcast_to(turned[None, :ROOM], out_ref.shape)


def bits_set(x):
    x = x - ((x >> 1) & 0x5555)
    x = (x & 0x3333) + ((x >> 2) & 0x3333)
    x = (x + (x >> 4)) & 0x0F0F
    return (x + (x >> 8)) & 0x1F


def index_kernel(tab_ref, cols_ref, starts_ref, map_ref, turned_ref):
    p0, c = place()
    spot = lax.broadcasted_iota(jnp.int32, (GROUPS * ROOM, NP), 1)
    parts = [tab_ref[GROUPS * n : GROUPS * (n + 1)] for n in range(NEAR // GROUPS)]
    turned = ((parts[0] + parts[1]) + (parts[2] + parts[3])).reshape(GROUPS * ROOM, NP)
    turned = (turned - spot + HP) & (NP - 1)
    turned_ref[...] = turned
    panel = lax.broadcasted_iota(jnp.int32, (1, NP), 1)
    wants = []
    owns = []
    for r in range(PB):
        want = jnp.zeros((1, NP), jnp.int32)
        for g in range(GROUPS):
            for s in range(KG):
                at = ROOM * g + KG * r + s
                want = want | jnp.left_shift(1, PB * turned_ref[at : at + 1, :] + g)
        wants.append(want)
        own = jnp.zeros((1, NP), jnp.int32)
        for s in range(KG):
            own = own | jnp.left_shift(1, turned_ref[pl.ds(ROOM * c + KG * r + s, 1), :])
        owns.append(own)
    pad = [jnp.zeros((PB, NP), jnp.int32)]
    want = jnp.concatenate(wants + pad, axis=0)
    own = jnp.concatenate(owns + pad, axis=0)
    found = jnp.zeros((8, NP), jnp.int32)
    for w in range(WIN):
        there = pltpu.roll(own, (HP - w) % NP, 1) if w != HP else own
        there = there << w
        for kr in range(PB):
            used = -((want >> (PB * w + kr)) & 1)
            found = found | (used & there[kr : kr + 1, :])
    counts = bits_set(found)
    before = jnp.sum(jnp.where(panel < p0, counts, 0).astype(jnp.float32)).astype(jnp.int32)
    here = jnp.where(panel == p0, 1, 0)
    mask = jnp.sum((found * here).astype(jnp.float32), axis=1, keepdims=True)
    count = jnp.sum((counts * here).astype(jnp.float32), axis=1, keepdims=True).astype(jnp.int32)
    mask = mask.astype(jnp.int32)
    lane = lax.broadcasted_iota(jnp.int32, (8, BS), 1)
    held = jnp.where(lane < 16, (jnp.broadcast_to(mask, (8, BS)) >> (lane & 15)) & 1, 0)
    turn = (2 * HP - p0) & (NP - 1)
    turn = jnp.where(turn > 14, 0, turn)
    col_of = lax.broadcasted_iota(jnp.int32, (BS, BS), 1)
    row_of = lax.broadcasted_iota(jnp.int32, (BS, BS), 0)
    ahead = ((row_of - turn) & 15) < ((col_of - turn) & 15)
    ahead = jnp.where(ahead, 1.0, 0.0).astype(jnp.bfloat16)
    rank = jnp.dot(held.astype(jnp.bfloat16), ahead, preferred_element_type=jnp.float32)
    rank = rank.astype(jnp.int32)
    slot = lax.broadcasted_iota(jnp.int32, (40, BS), 0)
    panels = ((p0 - 2 * HP + lane) & (NP - 1)).astype(jnp.bfloat16)
    slots = lax.broadcasted_iota(jnp.int32, (1, 40), 1)
    start = before
    for r in range(PB):
        taken = (rank[r : r + 1, :] == slot) & (held[r : r + 1, :] > 0)
        taken = jnp.where(taken, 1.0, 0.0).astype(jnp.bfloat16)
        col = lax.dot_general(
            panels, taken, (((1,), (1,)), ((), ())), preferred_element_type=jnp.float32
        )
        cols = jnp.where(slots < count[r : r + 1, :], PB * col[:1].astype(jnp.int32) + c, -1)
        cols_ref[r : r + 1, :] = cols[:, :WIDTH]
        starts_ref[:, r : r + 1] = jnp.broadcast_to(start, (1, 1))
        start = start + count[r : r + 1, :]
    window = lax.broadcasted_iota(jnp.int32, (2 * WIN, NP), 0)
    panels = lax.broadcasted_iota(jnp.int32, (2 * WIN, NP), 1)
    pick = jnp.where(panels == ((p0 - HP + window) & (NP - 1)), 1.0, 0.0).astype(jnp.bfloat16)
    near = lax.dot_general(
        pick,
        turned.astype(jnp.float32).astype(jnp.bfloat16),
        (((1,), (1,)), ((), ())),
        preferred_element_type=jnp.float32,
    )
    map_ref[:WIN, : GROUPS * ROOM] = near[:WIN].astype(jnp.int32)
    map_ref[WIN:, :] = rank


def square_kernel(
    map_ref, up_ref, over_ref, down_ref, trio_ref, swap_ref, back_ref, far_ref, out_ref, *refs
):
    rights, sums, staged, blank, in_sem, zero_sem, out_sem = refs
    p0, c = place()
    core = p0 & 1
    blank[...] = jnp.zeros(blank.shape, blank.dtype)
    for r in range(PB):
        pltpu.make_async_copy(blank, out_ref.at[r, USED:], zero_sem.at[r]).start()
    moves = (
        (trio_ref.at[0], HP, HP),
        (trio_ref.at[1], 2, 2),
        (trio_ref.at[2], 6, 6),
        (swap_ref.at[0], 5, 3),
        (swap_ref.at[1], 3, 1),
        (swap_ref.at[2], 7, 5),
        (back_ref, 0, 0),
        (far_ref, 1, 7),
    )
    copies = []
    for n, (ref, even, odd) in enumerate(moves):
        w = even if even == odd else jnp.where(core == 0, even, odd)
        copies.append(pltpu.make_async_copy(ref, rights.at[w], in_sem.at[n]))
    for copy in copies:
        copy.start()
    sums[...] = jnp.zeros(sums.shape, jnp.float32)
    for copy in copies:
        copy.wait()

    def row_step(r, carry):
        for d in range(GROUPS):
            g = (c + d) & (GROUPS - 1)
            left_ref = (trio_ref.at[0], up_ref, over_ref, down_ref)[d]
            for s0 in range(KG):
                w = map_ref[HP, ROOM * g + KG * r + s0]
                slots = []
                for s in range(KG):
                    slots.append(map_ref[WIN + r, map_ref[w, ROOM * c + KG * g + s] + w])
                right = jnp.concatenate([rights[w, g, s] for s in range(KG)], axis=1)
                product = jnp.dot(left_ref[r, s0], right, preferred_element_type=jnp.float32)
                new = [
                    sums[r, slots[s]] + product[:, BS * s : BS * (s + 1)] for s in range(KG)
                ]
                for s in range(KG):
                    sums[r, slots[s]] = new[s]
        staged[r] = sums[r].astype(jnp.bfloat16)
        pltpu.make_async_copy(staged.at[r], out_ref.at[r, :USED], out_sem.at[r]).start()
        return carry

    lax.fori_loop(0, PB, row_step, 0)
    for r in range(PB):
        pltpu.make_async_copy(blank, out_ref.at[r, USED:], zero_sem.at[r]).wait()
        pltpu.make_async_copy(staged.at[r], out_ref.at[r, :USED], out_sem.at[r]).wait()


VMEM = pl.BlockSpec(memory_space=pltpu.VMEM)
SMEM = pl.BlockSpec(memory_space=pltpu.SMEM)
HBM = pl.BlockSpec(memory_space=pl.ANY)


def near_core(array):
    return pltpu.with_memory_space_constraint(array, pltpu.VMEM)


def spread(cols):
    return pl.pallas_call(
        spread_kernel,
        out_shape=jax.ShapeDtypeStruct((FAR, 1, BS), jnp.int32),
        in_specs=[HBM],
        out_specs=VMEM,
        scratch_shapes=[pltpu.SMEM((KG, 1, PB), jnp.int32), pltpu.SemaphoreType.DMA],
        compiler_params=pltpu.CompilerParams(vmem_limit_bytes=8 << 20),
        name="spread",
    )(pltpu.with_memory_space_constraint(cols, pltpu.HBM))


def turned_table(parts):
    return pl.pallas_call(
        turn_kernel,
        out_shape=jax.ShapeDtypeStruct((NEAR, ROOM, BS), jnp.int32),
        in_specs=[VMEM],
        out_specs=VMEM,
        scratch_shapes=[pltpu.VMEM((NP, BS), jnp.int32)],
        compiler_params=pltpu.CompilerParams(vmem_limit_bytes=8 << 20),
        name="turned_table",
    )(parts)


def indices(table):
    return pl.pallas_call(
        index_kernel,
        out_shape=(
            jax.ShapeDtypeStruct((PB, WIDTH), jnp.int32),
            jax.ShapeDtypeStruct((1, PB), jnp.int32),
            jax.ShapeDtypeStruct((16, BS), jnp.int32),
        ),
        in_specs=[VMEM],
        out_specs=(VMEM, VMEM, VMEM),
        scratch_shapes=[pltpu.VMEM((GROUPS * ROOM, NP), jnp.int32)],
        compiler_params=pltpu.CompilerParams(vmem_limit_bytes=8 << 20),
        name="indices",
    )(table)


def square(where, lefts, pieces):
    return pl.pallas_call(
        square_kernel,
        out_shape=jax.ShapeDtypeStruct((PB, WIDTH, BS, BS), jnp.bfloat16),
        in_specs=[SMEM] + [VMEM] * (len(lefts) + len(pieces)),
        out_specs=HBM,
        scratch_shapes=[
            pltpu.VMEM((WIN, PB, KG, BS, BS), jnp.bfloat16),
            pltpu.VMEM((PB, USED, BS, BS), jnp.float32),
            pltpu.VMEM((PB, USED, BS, BS), jnp.bfloat16),
            pltpu.VMEM((WIDTH - USED, BS, BS), jnp.bfloat16),
            pltpu.SemaphoreType.DMA((WIN,)),
            pltpu.SemaphoreType.DMA((PB,)),
            pltpu.SemaphoreType.DMA((PB,)),
        ],
        compiler_params=pltpu.CompilerParams(vmem_limit_bytes=24 << 20),
        name="square",
    )(where, *[near_core(piece) for piece in (*lefts, *pieces)])


def exchange(array, axes):
    return lax.all_to_all(array, axes, 0, 0, tiled=True)


def swapped(block):
    return lax.ppermute(block, "rows_2", [(0, 1), (1, 0)])


def turned(block, distance):
    return lax.ppermute(block, "cols", [((c + distance) % GROUPS, c) for c in range(GROUPS)])


def sent_on(block, chips, crossed=False):
    count = NP // 2
    route = []
    for q in range(count):
        for core in range(2):
            step = chips * (2 * core - 1) if crossed else chips
            route.append((2 * q + core, 2 * ((q + step) % count) + (core ^ crossed)))
    return lax.ppermute(block, ROWS, route)


def on_device(blocks, block_cols):
    own = blocks[:, 0]
    parts = exchange(spread(block_cols.transpose(2, 1, 0)), FAR_AXES)
    table = exchange(turned_table(parts), NEAR_AXES)
    columns, starts, where = indices(table)
    behind = sent_on(own, 1)
    ahead = sent_on(own, -1)
    far = sent_on(own, 2, True)
    over = turned(own, 2)
    up = turned(own, 1)
    down = turned(own, 3)
    back = sent_on(behind, 1)
    trio = jnp.stack([own, behind, ahead])
    swap = swapped(trio)
    out = square(where, (up, over, down), (trio, swap, back, far))
    return out[:, None], columns[:, None], starts.reshape(PB, 1)


def solution(mesh):
    split = Mesh(
        mesh.devices.reshape(16, 4, 2, mesh.shape["cols"]), ("rows_0", "rows_1", "rows_2", "cols")
    )
    return jax.shard_map(
        on_device,
        mesh=split,
        in_specs=(P(ROWS, "cols", None, None, None), P(ROWS, "cols", None)),
        out_specs=(P(ROWS, "cols", None, None, None), P(ROWS, "cols", None), P(ROWS, "cols")),
        check_vma=False,
    )
```

```python
import jax
import jax.numpy as jnp
from jax import lax
from jax.experimental import pallas as pl
from jax.experimental.pallas import tpu as pltpu
from jax.sharding import Mesh
from jax.sharding import PartitionSpec as P

HP = 4
PB = 4
KG = 3
GROUPS = 4
BS = 128
NP = 128
WIDTH = 36
USED = 15
WIN = 2 * HP
ROWS = ("rows_0", "rows_1", "rows_2")
ROOM = 16
FAR = 64
NEAR = 8
FAR_AXES = ("rows_0", "rows_1")
NEAR_AXES = ("rows_2", "cols")


def place():
    return lax.axis_index(ROWS), lax.axis_index("cols")


def spread_kernel(held_ref, out_ref, cols_ref, sem):
    copy = pltpu.make_async_copy(held_ref, cols_ref, sem)
    copy.start()
    copy.wait()
    lane = lax.broadcasted_iota(jnp.int32, (1, BS), 1)
    row = jnp.zeros((1, BS), jnp.int32)
    for r in range(PB):
        for s in range(KG):
            row = jnp.where(lane == KG * r + s, cols_ref[s, 0, r] >> 2, row)
    out_ref[...] = jnp.broadcast_to(row[None], out_ref.shape)


def turn_kernel(in_ref, out_ref, table_ref):
    p0, _ = place()
    table_ref[...] = jnp.zeros((NP, BS), jnp.int32)
    for n in range(FAR):
        spot = 2 * n + (p0 & 1)
        table_ref[pl.ds(spot, 1), :] = in_ref[n]
    turned = jnp.transpose(table_ref[...])[:ROOM].astype(jnp.float32).astype(jnp.bfloat16)
    out_ref[...] = jnp.broadcast_to(turned[None], out_ref.shape)


def bits_set(x):
    x = x - ((x >> 1) & 0x5555)
    x = (x & 0x3333) + ((x >> 2) & 0x3333)
    x = (x + (x >> 4)) & 0x0F0F
    return (x + (x >> 8)) & 0x1F


def index_kernel(tab_ref, cols_ref, starts_ref, map_ref, turned_ref):
    p0, c = place()
    spot = lax.broadcasted_iota(jnp.int32, (GROUPS * ROOM, NP), 1)
    parts = [tab_ref[GROUPS * n : GROUPS * (n + 1)].astype(jnp.float32) for n in range(2)]
    turned = (parts[0] + parts[1]).astype(jnp.int32).reshape(GROUPS * ROOM, NP)
    turned = (turned - spot + HP) & (NP - 1)
    turned_ref[...] = turned
    panel = lax.broadcasted_iota(jnp.int32, (1, NP), 1)
    wants = []
    owns = []
    for r in range(PB):
        want = jnp.zeros((1, NP), jnp.int32)
        for g in range(GROUPS):
            for s in range(KG):
                at = ROOM * g + KG * r + s
                want = want | jnp.left_shift(1, PB * turned_ref[at : at + 1, :] + g)
        wants.append(want)
        own = jnp.zeros((1, NP), jnp.int32)
        for s in range(KG):
            own = own | jnp.left_shift(1, turned_ref[pl.ds(ROOM * c + KG * r + s, 1), :])
        owns.append(own)
    pad = [jnp.zeros((PB, NP), jnp.int32)]
    want = jnp.concatenate(wants + pad, axis=0)
    own = jnp.concatenate(owns + pad, axis=0)
    found = jnp.zeros((8, NP), jnp.int32)
    for w in range(WIN):
        there = pltpu.roll(own, (HP - w) % NP, 1) if w != HP else own
        there = there << w
        for kr in range(PB):
            used = -((want >> (PB * w + kr)) & 1)
            found = found | (used & there[kr : kr + 1, :])
    counts = bits_set(found)
    before = jnp.sum(jnp.where(panel < p0, counts, 0).astype(jnp.float32)).astype(jnp.int32)
    here = jnp.where(panel == p0, 1, 0)
    mask = jnp.sum((found * here).astype(jnp.float32), axis=1, keepdims=True)
    count = jnp.sum((counts * here).astype(jnp.float32), axis=1, keepdims=True).astype(jnp.int32)
    mask = mask.astype(jnp.int32)
    lane = lax.broadcasted_iota(jnp.int32, (8, BS), 1)
    held = jnp.where(lane < 16, (jnp.broadcast_to(mask, (8, BS)) >> (lane & 15)) & 1, 0)
    turn = (2 * HP - p0) & (NP - 1)
    turn = jnp.where(turn > 14, 0, turn)
    col_of = lax.broadcasted_iota(jnp.int32, (BS, BS), 1)
    row_of = lax.broadcasted_iota(jnp.int32, (BS, BS), 0)
    ahead = ((row_of - turn) & 15) < ((col_of - turn) & 15)
    ahead = jnp.where(ahead, 1.0, 0.0).astype(jnp.bfloat16)
    rank = jnp.dot(held.astype(jnp.bfloat16), ahead, preferred_element_type=jnp.float32)
    rank = rank.astype(jnp.int32)
    slot = lax.broadcasted_iota(jnp.int32, (40, BS), 0)
    panels = ((p0 - 2 * HP + lane) & (NP - 1)).astype(jnp.bfloat16)
    slots = lax.broadcasted_iota(jnp.int32, (1, 40), 1)
    start = before
    for r in range(PB):
        taken = (rank[r : r + 1, :] == slot) & (held[r : r + 1, :] > 0)
        taken = jnp.where(taken, 1.0, 0.0).astype(jnp.bfloat16)
        col = lax.dot_general(
            panels, taken, (((1,), (1,)), ((), ())), preferred_element_type=jnp.float32
        )
        cols = jnp.where(slots < count[r : r + 1, :], PB * col[:1].astype(jnp.int32) + c, -1)
        cols_ref[r : r + 1, :] = cols[:, :WIDTH]
        starts_ref[:, r : r + 1] = jnp.broadcast_to(start, (1, 1))
        start = start + count[r : r + 1, :]
    window = lax.broadcasted_iota(jnp.int32, (2 * WIN, NP), 0)
    panels = lax.broadcasted_iota(jnp.int32, (2 * WIN, NP), 1)
    pick = jnp.where(panels == ((p0 - HP + window) & (NP - 1)), 1.0, 0.0).astype(jnp.bfloat16)
    near = lax.dot_general(
        pick,
        turned.astype(jnp.float32).astype(jnp.bfloat16),
        (((1,), (1,)), ((), ())),
        preferred_element_type=jnp.float32,
    )
    map_ref[:WIN, : GROUPS * ROOM] = near[:WIN].astype(jnp.int32)
    map_ref[WIN:, :] = rank


def square_kernel(
    map_ref, up_ref, over_ref, down_ref, trio_ref, swap_ref, back_ref, far_ref, out_ref, *refs
):
    rights, sums, staged, blank, in_sem, zero_sem, out_sem = refs
    p0, c = place()
    core = p0 & 1
    blank[...] = jnp.zeros(blank.shape, blank.dtype)
    for r in range(PB):
        pltpu.make_async_copy(blank, out_ref.at[r, USED:], zero_sem.at[r]).start()
    moves = (
        (trio_ref.at[0], HP, HP),
        (trio_ref.at[1], 2, 2),
        (trio_ref.at[2], 6, 6),
        (swap_ref.at[0], 5, 3),
        (swap_ref.at[1], 3, 1),
        (swap_ref.at[2], 7, 5),
        (back_ref, 0, 0),
        (far_ref, 1, 7),
    )
    copies = []
    for n, (ref, even, odd) in enumerate(moves):
        w = even if even == odd else jnp.where(core == 0, even, odd)
        copies.append(pltpu.make_async_copy(ref, rights.at[w], in_sem.at[n]))
    for copy in copies:
        copy.start()
    sums[...] = jnp.zeros(sums.shape, jnp.float32)
    for copy in copies:
        copy.wait()

    def row_step(r, carry):
        for d in range(GROUPS):
            g = (c + d) & (GROUPS - 1)
            left_ref = (trio_ref.at[0], up_ref, over_ref, down_ref)[d]
            for s0 in range(KG):
                w = map_ref[HP, ROOM * g + KG * r + s0]
                slots = []
                for s in range(KG):
                    slots.append(map_ref[WIN + r, map_ref[w, ROOM * c + KG * g + s] + w])
                right = jnp.concatenate([rights[w, g, s] for s in range(KG)], axis=1)
                product = jnp.dot(left_ref[r, s0], right, preferred_element_type=jnp.float32)
                new = [
                    sums[r, slots[s]] + product[:, BS * s : BS * (s + 1)] for s in range(KG)
                ]
                for s in range(KG):
                    sums[r, slots[s]] = new[s]
        staged[r] = sums[r].astype(jnp.bfloat16)
        pltpu.make_async_copy(staged.at[r], out_ref.at[r, :USED], out_sem.at[r]).start()
        return carry

    lax.fori_loop(0, PB, row_step, 0)
    for r in range(PB):
        pltpu.make_async_copy(blank, out_ref.at[r, USED:], zero_sem.at[r]).wait()
        pltpu.make_async_copy(staged.at[r], out_ref.at[r, :USED], out_sem.at[r]).wait()


VMEM = pl.BlockSpec(memory_space=pltpu.VMEM)
SMEM = pl.BlockSpec(memory_space=pltpu.SMEM)
HBM = pl.BlockSpec(memory_space=pl.ANY)


def near_core(array):
    return pltpu.with_memory_space_constraint(array, pltpu.VMEM)


def spread(cols):
    return pl.pallas_call(
        spread_kernel,
        out_shape=jax.ShapeDtypeStruct((FAR, 1, BS), jnp.int32),
        in_specs=[HBM],
        out_specs=VMEM,
        scratch_shapes=[pltpu.SMEM((KG, 1, PB), jnp.int32), pltpu.SemaphoreType.DMA],
        compiler_params=pltpu.CompilerParams(vmem_limit_bytes=8 << 20),
        name="spread",
    )(pltpu.with_memory_space_constraint(cols, pltpu.HBM))


def turned_table(parts):
    return pl.pallas_call(
        turn_kernel,
        out_shape=jax.ShapeDtypeStruct((NEAR, ROOM, BS), jnp.bfloat16),
        in_specs=[VMEM],
        out_specs=VMEM,
        scratch_shapes=[pltpu.VMEM((NP, BS), jnp.int32)],
        compiler_params=pltpu.CompilerParams(vmem_limit_bytes=8 << 20),
        name="turned_table",
    )(parts)


def indices(table):
    return pl.pallas_call(
        index_kernel,
        out_shape=(
            jax.ShapeDtypeStruct((PB, WIDTH), jnp.int32),
            jax.ShapeDtypeStruct((1, PB), jnp.int32),
            jax.ShapeDtypeStruct((16, BS), jnp.int32),
        ),
        in_specs=[VMEM],
        out_specs=(VMEM, VMEM, VMEM),
        scratch_shapes=[pltpu.VMEM((GROUPS * ROOM, NP), jnp.int32)],
        compiler_params=pltpu.CompilerParams(vmem_limit_bytes=8 << 20),
        name="indices",
    )(near_core(table))


def square(where, lefts, pieces):
    return pl.pallas_call(
        square_kernel,
        out_shape=jax.ShapeDtypeStruct((PB, WIDTH, BS, BS), jnp.bfloat16),
        in_specs=[SMEM] + [VMEM] * (len(lefts) + len(pieces)),
        out_specs=HBM,
        scratch_shapes=[
            pltpu.VMEM((WIN, PB, KG, BS, BS), jnp.bfloat16),
            pltpu.VMEM((PB, USED, BS, BS), jnp.float32),
            pltpu.VMEM((PB, USED, BS, BS), jnp.bfloat16),
            pltpu.VMEM((WIDTH - USED, BS, BS), jnp.bfloat16),
            pltpu.SemaphoreType.DMA((WIN,)),
            pltpu.SemaphoreType.DMA((PB,)),
            pltpu.SemaphoreType.DMA((PB,)),
        ],
        compiler_params=pltpu.CompilerParams(vmem_limit_bytes=24 << 20),
        name="square",
    )(where, *[near_core(piece) for piece in (*lefts, *pieces)])


def exchange(array, axes):
    return lax.all_to_all(array, axes, 0, 0, tiled=True)


def swapped(block):
    return lax.ppermute(block, "rows_2", [(0, 1), (1, 0)])


def turned(block, distance):
    return lax.ppermute(block, "cols", [((c + distance) % GROUPS, c) for c in range(GROUPS)])


def sent_on(block, chips, crossed=False):
    count = NP // 2
    route = []
    for q in range(count):
        for core in range(2):
            step = chips * (2 * core - 1) if crossed else chips
            route.append((2 * q + core, 2 * ((q + step) % count) + (core ^ crossed)))
    return lax.ppermute(block, ROWS, route)


def on_device(blocks, block_cols):
    own = blocks[:, 0]
    parts = exchange(spread(block_cols.transpose(2, 1, 0)), FAR_AXES)
    table = exchange(turned_table(parts), NEAR_AXES)
    columns, starts, where = indices(table)
    behind = sent_on(own, 1)
    ahead = sent_on(own, -1)
    far = sent_on(own, 2, True)
    over = turned(own, 2)
    up = turned(own, 1)
    down = turned(own, 3)
    back = sent_on(behind, 1)
    trio = jnp.stack([own, behind, ahead])
    swap = swapped(trio)
    out = square(where, (up, over, down), (trio, swap, back, far))
    return out[:, None], columns[:, None], starts.reshape(PB, 1)


def solution(mesh):
    split = Mesh(
        mesh.devices.reshape(16, 4, 2, mesh.shape["cols"]), ("rows_0", "rows_1", "rows_2", "cols")
    )
    return jax.shard_map(
        on_device,
        mesh=split,
        in_specs=(P(ROWS, "cols", None, None, None), P(ROWS, "cols", None)),
        out_specs=(P(ROWS, "cols", None, None, None), P(ROWS, "cols", None), P(ROWS, "cols")),
        check_vma=False,
    )
```
